256 devices in a mesh: gx: 16 (over z, x_lo), gy: 4 (over y), gz: 4 (over x_hi, core).
Axes of the slice: x: 4 (x_hi: 2, x_lo: 2; x = x_hi * 2 + x_lo), y: 4, z: 8, core: 2. Of those that a mesh axis runs over, the one named last changes fastest.
Arguments:
- state: float32 [5, 96, 96, 1536], P(None, 'gx', 'gy', 'gz'), as said below
- register: float32 [5, 96, 96, 1536], P(None, 'gx', 'gy', 'gz'), may hold values from -0.25 to 0.25
Outputs:
- new_state: float32 [5, 96, 96, 1536], P(None, 'gx', 'gy', 'gz')
- new_register: float32 [5, 96, 96, 1536], P(None, 'gx', 'gy', 'gz')
The draws below stay inside these ranges and needn't reach their ends.
Inputs may be any that keep to these rules, and one draw needn't show every extreme that they name: Density is between 0.5 and 2.5, and the pressure computed from the state is positive.
All inputs are finite; a program needn't handle non-finite values.
Results may differ from the reference program's by a relative error of at most 0.0003.
Values sent between devices are 32-bit elements; how exact they have to be, the bound alone decides.
A program may use at most 128 MiB of HBM per device.

```python
import math
import jax
import jax.numpy as jnp
import numpy as np
from jax import lax

NVAR = 5
NXN = 96
NYN = 96
NZN = 1536


def smooth_field(key, grid, amplitude):
    xpos = lax.broadcasted_iota(jnp.float32, grid, 0) / grid[0]
    ypos = lax.broadcasted_iota(jnp.float32, grid, 1) / grid[1]
    zpos = lax.broadcasted_iota(jnp.float32, grid, 2) / grid[2]
    waves = jax.random.randint(jax.random.fold_in(key, 1), (4, 3), 1, 4).astype(jnp.float32)
    phases = jax.random.uniform(jax.random.fold_in(key, 2), (4,), jnp.float32, 0.0, 6.283185307179586)
    total = jnp.zeros(grid, jnp.float32)
    for mode in range(4):
        angle = 6.283185307179586 * (waves[mode, 0] * xpos + waves[mode, 1] * ypos + waves[mode, 2] * zpos) + phases[mode]
        total = total + amplitude * jnp.sin(angle)
    return total


def draw_state(key, part):
    key_rho = jax.random.fold_in(key, 11)
    key_vel = jax.random.fold_in(key, 12)
    key_press = jax.random.fold_in(key, 13)
    grid = (NXN, NYN, NZN)
    xpos = lax.broadcasted_iota(jnp.float32, grid, 0) / NXN
    amp = 1.0 + 2.0 * xpos
    noise = 0.015 * jnp.clip(jax.random.normal(jax.random.fold_in(key_vel, 5), (3,) + grid, jnp.float32), -3.0, 3.0)
    rho_noise = 0.03 * jnp.clip(jax.random.normal(jax.random.fold_in(key_rho, 5), grid, jnp.float32), -3.0, 3.0)
    press_noise = 0.03 * jnp.clip(jax.random.normal(jax.random.fold_in(key_press, 5), grid, jnp.float32), -3.0, 3.0)
    density = 1.0 + smooth_field(key_rho, grid, 0.08) + rho_noise
    press = 1.0 + smooth_field(key_press, grid, 0.08) + press_noise
    vel = jnp.stack([amp * smooth_field(jax.random.fold_in(key_vel, c), grid, 0.1) for c in range(3)]) + noise
    energy = press / 0.4 + 0.5 * density * jnp.sum(vel * vel, axis=0)
    return jnp.concatenate([density[None], density[None] * vel, energy[None]], axis=0).astype(jnp.float32)


def block_scale(rng, extent, pieces, smallest, high):
    loudness = 1.0
    for axis_at, blocks in pieces:
        heights = jax.random.uniform(jax.random.fold_in(jax.random.fold_in(rng, 6), axis_at), (blocks,), jnp.float32, smallest / len(pieces), high / len(pieces))
        loudness = loudness * jnp.repeat(jnp.exp(heights), extent[axis_at] // blocks).reshape((-1,) + (1,) * (len(extent) - 1 - axis_at))
    return loudness


def centred(stream_key, shape, deviation, limit, cuts=(), dtype=jnp.bfloat16):
    result = deviation * jax.random.normal(stream_key, shape, jnp.float32)
    if cuts:
        result = result * block_scale(stream_key, shape, cuts, -0.22, 0.18)
    return jnp.clip(result, -limit, limit).astype(dtype)


def setup_inputs(seed: int = 0) -> dict:
    splits = jax.random.split(jax.random.key(seed), 3)
    state = draw_state(jax.random.fold_in(splits[2], 71), 0)
    register = centred(splits[1], (NVAR, NXN, NYN, NZN), 0.05, 0.25, ((1, 16), (2, 4), (3, 4)), jnp.float32)
    return dict(state=state, register=register)


GAMMA = 1.4
GM1 = 0.4
ELEM_WIDTH = 0.05
COURANT = 0.5
INV_W = 15.0
COEFFS = ((-567301805773.0 / 1357537059087.0, 5161836677717.0 / 13612068292357.0), (-2404267990393.0 / 2016746695238.0, 1720146321549.0 / 2090206949498.0))
FORMS = ('ij,vejyz->veiyz', 'ij,vxejz->vxeiz', 'ij,vxyej->vxyei')

def gll_derivative():
    seven = math.sqrt(7.0)
    inner = math.sqrt(1.0 / 3.0 - 2.0 * seven / 21.0)
    outer = math.sqrt(1.0 / 3.0 + 2.0 * seven / 21.0)
    points = np.array([-1.0, -outer, -inner, inner, outer, 1.0])
    count = len(points)
    weights = np.array([np.prod([points[i] - points[j] for j in range(count) if j != i]) for i in range(count)])
    table = np.zeros((count, count))
    for i in range(count):
        for j in range(count):
            if i != j:
                table[i, j] = weights[i] / weights[j] / (points[i] - points[j])
        table[i, i] = -np.sum(table[i])
    return table

def pressure(u):
    mom_sq = u[1] * u[1] + u[2] * u[2] + u[3] * u[3]
    return (GM1 * (u[4] - 0.5 * mom_sq / u[0]), mom_sq)

def euler_flux(u, d):
    press, mom_sq = pressure(u)
    vel = u[1 + d] / u[0]
    parts = [u[1 + d], u[1] * vel, u[2] * vel, u[3] * vel, (u[4] + press) * vel]
    parts[1 + d] = parts[1 + d] + press
    speed = jnp.abs(vel) + jnp.sqrt(GAMMA * press / u[0])
    return (jnp.stack(parts), speed)

def direction_term(ext, d, diff):
    axis = 1 + d
    nodes = diff.shape[0]
    full = ext.shape[axis]
    length = full - 2
    elems = length // nodes
    inner = lax.slice_in_dim(ext, 1, full - 1, axis=axis)
    flux_in, unused = euler_flux(inner, d)
    shape = flux_in.shape
    blocked = flux_in.reshape(shape[:axis] + (elems, nodes) + shape[axis + 1:])
    deriv = jnp.einsum(FORMS[d], diff, blocked, precision=lax.Precision.HIGHEST).reshape(shape)
    lower_side = lax.slice_in_dim(ext, 0, length + 1, nodes, axis)
    upper_side = lax.slice_in_dim(ext, 1, length + 2, nodes, axis)
    flux_low, speed_low = euler_flux(lower_side, d)
    flux_up, speed_up = euler_flux(upper_side, d)
    lam = jnp.maximum(speed_low, speed_up)
    fstar = 0.5 * (flux_low + flux_up) - 0.5 * lam[None] * (upper_side - lower_side)
    first = lax.slice_in_dim(flux_in, 0, length, nodes, axis)
    last = lax.slice_in_dim(flux_in, nodes - 1, length, nodes, axis)
    lower = -(first - lax.slice_in_dim(fstar, 0, elems, axis=axis)) * INV_W
    upper = (last - lax.slice_in_dim(fstar, 1, elems + 1, axis=axis)) * INV_W
    bshape = shape[:axis] + (elems, 1) + shape[axis + 1:]
    zeros = jnp.zeros(shape[:axis] + (elems, nodes - 2) + shape[axis + 1:], jnp.float32)
    corr = jnp.concatenate([lower.reshape(bshape), zeros, upper.reshape(bshape)], axis=axis + 1).reshape(shape)
    return 2.0 / ELEM_WIDTH * (corr - deriv)

def max_speed(u):
    press, mom_sq = pressure(u)
    return jnp.max(jnp.sqrt(mom_sq) / u[0] + jnp.sqrt(GAMMA * press / u[0]))

def residual_of(u, diff):
    total = jnp.zeros_like(u)
    for d in range(3):
        pads = [(0, 0)] * 4
        pads[1 + d] = (1, 1)
        ext = jnp.pad(u, pads, mode='wrap')
        total = total + direction_term(ext, d, diff)
    return total

def reference(state, register):
    diff = jnp.asarray(gll_derivative(), jnp.float32)
    step = COURANT * ELEM_WIDTH / (11.0 * max_speed(state))
    current = state
    section_reg = register
    for coef_a, coef_b in COEFFS:
        section_reg = coef_a * section_reg + step * residual_of(current, diff)
        current = current + coef_b * section_reg
    return (current, section_reg)
```

```python
import functools
import math

import jax
import jax.numpy as jnp
import numpy as np
from jax import lax
from jax.experimental import pallas as pl
from jax.experimental.pallas import tpu as pltpu
from jax.sharding import Mesh
from jax.sharding import PartitionSpec as P

AXES = ("gx_0", "gx_1", "gy", "gz_0", "gz_1")
MESH = pl.DeviceIdType.MESH

GAMMA = 1.4
GM1 = 0.4
ELEM_WIDTH = 0.05
COURANT = 0.5
COEFFS = (
    (-567301805773.0 / 1357537059087.0, 5161836677717.0 / 13612068292357.0),
    (-2404267990393.0 / 2016746695238.0, 1720146321549.0 / 2090206949498.0),
)
NV = 5
N = 6
NX, NY, NZ = 6, 24, 384
ROWS = 8
CH = NY // ROWS
LANES = 128
SCALE = 2.0 / ELEM_WIDTH
FACE = SCALE * 15.0 * 0.5


def gll_derivative():
    seven = math.sqrt(7.0)
    inner = math.sqrt(1.0 / 3.0 - 2.0 * seven / 21.0)
    outer = math.sqrt(1.0 / 3.0 + 2.0 * seven / 21.0)
    points = np.array([-1.0, -outer, -inner, inner, outer, 1.0])
    count = len(points)
    weights = np.array(
        [np.prod([points[i] - points[j] for j in range(count) if j != i]) for i in range(count)]
    )
    table = np.zeros((count, count))
    for i in range(count):
        for j in range(count):
            if i != j:
                table[i, j] = weights[i] / weights[j] / (points[i] - points[j])
        table[i, i] = -np.sum(table[i])
    return table


DIFF = gll_derivative()


def line_operator(length):
    elems = length // N
    op = np.kron(np.eye(elems), -SCALE * DIFF)
    for e in range(elems - 1):
        last, first = N * e + N - 1, N * e + N
        for row in (last, first):
            op[row, last] += FACE
            op[row, first] -= FACE
    return op


def operators():
    along_z = line_operator(NZ).T
    cut = 2 * LANES - (2 * LANES) % N
    low = along_z[: 2 * LANES, : 2 * LANES].copy()
    low[:, cut:] = 0.0
    high = along_z[LANES:, LANES:].copy()
    high[:, : cut - LANES] = 0.0
    along_y = np.kron(np.eye(NX), line_operator(NY))
    return (
        jnp.asarray(np.stack([low, high]), jnp.float32),
        jnp.asarray(along_y, jnp.float32),
    )


def primitives(u):
    inv = 1.0 / u[0]
    vel = [u[1] * inv, u[2] * inv, u[3] * inv]
    press = GM1 * (u[4] - 0.5 * (u[1] * vel[0] + u[2] * vel[1] + u[3] * vel[2]))
    sound = jnp.sqrt(GAMMA * press * inv)
    return vel, press, sound


def flux(u, vel, press, d):
    parts = [u[1 + d], u[1] * vel[d], u[2] * vel[d], u[3] * vel[d], (u[4] + press) * vel[d]]
    parts[1 + d] = parts[1 + d] + press
    return parts


def face_terms(left, right, d):
    vel_l, press_l, sound_l = primitives(left)
    vel_r, press_r, sound_r = primitives(right)
    flux_l = flux(left, vel_l, press_l, d)
    flux_r = flux(right, vel_r, press_r, d)
    lam = FACE * jnp.maximum(jnp.abs(vel_l[d]) + sound_l, jnp.abs(vel_r[d]) + sound_r)
    a = [FACE * (fl - fr) for fl, fr in zip(flux_l, flux_r)]
    b = [lam * (r - l) for l, r in zip(left, right)]
    return a, b


def kernel(
    sizes,
    state,
    register,
    mat_z,
    mat_y,
    out_state,
    out_register,
    u,
    k,
    res,
    fx,
    fy,
    fz,
    mz,
    my,
    mask_z,
    step,
    top,
    top_x,
    top_z,
    top_y,
    y_pack,
    z_pack,
    y_halo,
    z_halo,
    x_halo,
    y_corr,
    z_corr,
    load_sem,
    send_x,
    recv_x,
    send_yz,
    recv_yz,
    send_top,
    recv_top,
):
    nz, nxl, ny, nxh, nco = sizes
    z, xl, y, xh, co = (lax.axis_index(a) for a in AXES)

    def device(z_=z, xl_=xl, y_=y, xh_=xh, co_=co):
        return dict(zip(AXES, (z_, xl_, y_, xh_, co_)))

    def wrap(i, n):
        return lax.rem(i + n, n)

    other_xl, other_co = wrap(xl + 1, nxl), wrap(co + 1, nco)
    gx = (
        device(z_=wrap(z + xl - 1, nz), xl_=other_xl),
        device(z_=wrap(z + xl, nz), xl_=other_xl),
    )
    gy = (device(y_=wrap(y - 1, ny)), device(y_=wrap(y + 1, ny)))
    gz = (
        device(xh_=wrap(xh + co - 1, nxh), co_=other_co),
        device(xh_=wrap(xh + co, nxh), co_=other_co),
    )
    group_x = [
        device(xh_=wrap(xh + a, nxh), xl_=wrap(xl + b, nxl), co_=wrap(co + c, nco))
        for a in range(nxh)
        for b in range(nxl)
        for c in range(nco)
        if a or b or c
    ]
    group_z = [device(z_=wrap(z + i, nz)) for i in range(1, nz)]
    group_y = [device(y_=wrap(y + i, ny)) for i in range(1, ny)]
    diagonal = device(z_=wrap(z + 2 * xl - 1, nz), xl_=other_xl)

    loads = [
        pltpu.make_async_copy(state, u, load_sem.at[0]),
        pltpu.make_async_copy(register, k, load_sem.at[1]),
        pltpu.make_async_copy(mat_z, mz, load_sem.at[2]),
        pltpu.make_async_copy(mat_y, my, load_sem.at[3]),
    ]
    for load in loads:
        load.start()
    barrier = pltpu.get_barrier_semaphore()
    partners = group_x + group_z + group_y + [diagonal]
    for partner in partners:
        pl.semaphore_signal(barrier, inc=1, device_id=partner, device_id_type=MESH)

    lane = lax.broadcasted_iota(jnp.int32, (ROWS, NZ), 1)
    lane_f = lane.astype(jnp.float32)
    place = lane_f - N * jnp.floor((lane_f + 0.5) * (1.0 / N))
    mask_z[...] = jnp.where((place > N - 1.5) & (lane < NZ - 1), FACE, 0.0)
    row = lax.broadcasted_iota(jnp.int32, (ROWS, NZ), 0)
    lane_1 = lax.broadcasted_iota(jnp.int32, (NY, LANES), 1)

    def chunk(ref, x, c):
        return [ref[v, x, pl.ds(ROWS * c, ROWS), :] for v in range(NV)]

    loads[0].wait()
    top[0] = jnp.zeros((ROWS, LANES), jnp.float32)

    def speed_body(x, carry):
        for c in range(CH):
            w = chunk(u, x, c)
            vel, press, sound = primitives(w)
            mom = jnp.sqrt(w[1] * w[1] + w[2] * w[2] + w[3] * w[3])
            s = mom * (1.0 / w[0]) + sound
            carry = jnp.maximum(carry, s)
        return carry

    best = lax.fori_loop(0, NX, speed_body, jnp.zeros((ROWS, NZ), jnp.float32))
    top[0] = jnp.maximum(
        jnp.maximum(best[:, :LANES], best[:, LANES : 2 * LANES]), best[:, 2 * LANES :]
    )

    def pack(sec):
        def body(v, carry):
            low, high = carry
            for x in range(NX):
                y_pack[sec, 0, v, x : x + 1, :] = u[v, x, 0:1, :]
                y_pack[sec, 1, v, x : x + 1, :] = u[v, x, NY - 1 : NY, :]
                here = lane_1 == v * NX + x
                low = jnp.where(here, u[v, x, :, 0:LANES][:, 0:1], low)
                high = jnp.where(here, u[v, x, :, NZ - LANES : NZ][:, LANES - 1 : LANES], high)
            for x in range(NX, ROWS):
                y_pack[sec, 0, v, x : x + 1, :] = u[v, 0, 0:1, :]
                y_pack[sec, 1, v, x : x + 1, :] = u[v, 0, NY - 1 : NY, :]
            return low, high

        ones = jnp.ones((NY, LANES), jnp.float32)
        low, high = lax.fori_loop(0, NV, body, (ones, ones))
        z_pack[sec, 0] = low
        z_pack[sec, 1] = high

    def remote(src, dst, send, recv, to):
        return pltpu.make_async_remote_copy(
            src_ref=src,
            dst_ref=dst,
            send_sem=send,
            recv_sem=recv,
            device_id=to,
            device_id_type=MESH,
        )

    def x_copy(sec, side, c):
        src = state if sec == 0 else u
        return remote(
            src.at[:, 0 if side == 0 else NX - 1, pl.ds(ROWS * c, ROWS), :],
            x_halo.at[sec, 1 - side, c],
            send_x.at[sec, side, c],
            recv_x.at[sec, 1 - side, c],
            gx[side],
        )

    def y_copy(sec, side):
        return remote(
            y_pack.at[sec, side],
            y_halo.at[sec, 1 - side],
            send_yz.at[sec, 0, side],
            recv_yz.at[sec, 0, 1 - side],
            gy[side],
        )

    def z_copy(sec, side):
        return remote(
            z_pack.at[sec, side],
            z_halo.at[sec, 1 - side],
            send_yz.at[sec, 1, side],
            recv_yz.at[sec, 1, 1 - side],
            gz[side],
        )

    def top_copies(stage, group, slots, first):
        return [
            remote(top.at[stage], slots.at[i], send_top.at[first + i], recv_top.at[first + i], to)
            for i, to in enumerate(group)
        ]

    tops_x = top_copies(0, group_x, top_x, 0)
    tops_z = top_copies(1, group_z, top_z, len(group_x))
    tops_y = top_copies(2, group_y, top_y, len(group_x) + len(group_z))

    def start(copies):
        for copy in copies:
            copy.start()

    def gather_top(stage, copies, slots):
        value = top[stage]
        for i, copy in enumerate(copies):
            copy.wait_recv()
            value = jnp.maximum(value, slots[i])
        return value

    def y_z_copies(sec):
        return [z_copy(sec, 0), z_copy(sec, 1), y_copy(sec, 0), y_copy(sec, 1)]

    def fluxes_and_jumps():
        def body(x, carry):
            for c in range(CH):
                w = chunk(u, x, c)
                vel, press, sound = primitives(w)
                rows = pl.ds(ROWS * c, ROWS)
                for d, to in enumerate((fx, fy, fz)):
                    for v, part in enumerate(flux(w, vel, press, d)):
                        to[v, x, rows, :] = part
                s_y = jnp.abs(vel[1]) + sound
                s_z = jnp.abs(vel[2]) + sound
                lam_y = jnp.where(
                    row == N - 1 - 2 * c,
                    FACE * jnp.maximum(s_y, pltpu.roll(s_y, ROWS - 1, 0)),
                    0.0,
                )
                lam_z = mask_z[...] * jnp.maximum(s_z, pltpu.roll(s_z, NZ - 1, 1))
                for v in range(NV):
                    t_y = lam_y * (pltpu.roll(w[v], ROWS - 1, 0) - w[v])
                    t_z = lam_z * (pltpu.roll(w[v], NZ - 1, 1) - w[v])
                    res[v, x, rows, :] = (t_y - pltpu.roll(t_y, 1, 0)) + (
                        t_z - pltpu.roll(t_z, 1, 1)
                    )
            return carry

        lax.fori_loop(0, NX, body, 0)

    def dot(a, b):
        return jnp.dot(
            a, b, precision=lax.Precision.HIGHEST, preferred_element_type=jnp.float32
        )

    def lines_y_z():
        def body(v, carry):
            along_z = fz[v].reshape(NX * NY, NZ)
            low = dot(along_z[:, : 2 * LANES], mz[0])
            high = dot(along_z[:, LANES:], mz[1])
            both = jnp.concatenate(
                [low[:, :LANES], low[:, LANES:] + high[:, :LANES], high[:, LANES:]], axis=1
            )
            along_y = dot(my[...], fy[v].reshape(NX * NY, NZ))
            res[v] = res[v] + (both + along_y).reshape(NX, NY, NZ)
            return carry

        lax.fori_loop(0, NV, body, 0)

    def lines_x():
        half = N // 2
        even = [[-SCALE * 0.5 * (DIFF[i, j] + DIFF[i, N - 1 - j]) for j in range(half)] for i in range(half)]
        odd = [[-SCALE * 0.5 * (DIFF[i, j] - DIFF[i, N - 1 - j]) for j in range(half)] for i in range(half)]

        def body(v, carry):
            for c in range(CH):
                rows = pl.ds(ROWS * c, ROWS)
                f = [fx[v, x, rows, :] for x in range(NX)]
                plus = [f[j] + f[N - 1 - j] for j in range(half)]
                minus = [f[j] - f[N - 1 - j] for j in range(half)]
                for i in range(half):
                    a = sum(even[i][j] * plus[j] for j in range(half))
                    b = sum(odd[i][j] * minus[j] for j in range(half))
                    res[v, i, rows, :] += b + a
                    res[v, N - 1 - i, rows, :] += b - a
            return carry

        lax.fori_loop(0, NV, body, 0)

    def y_z_faces(sec):
        for side in (0, 1):
            y_copy(sec, 1 - side).wait_recv()
            own = [y_pack[sec, side, v] for v in range(NV)]
            far = [y_halo[sec, side, v] for v in range(NV)]
            a, b = face_terms(far, own, 1) if side == 0 else face_terms(own, far, 1)
            for v in range(NV):
                y_corr[side, v] = a[v] - b[v] if side == 0 else a[v] + b[v]
            z_copy(sec, 1 - side).wait_recv()

            def part(ref, v):
                tile = ref[sec, side]
                return tile if v == 0 else pltpu.roll(tile, LANES - NX * v, 1)

            own = [part(z_pack, v) for v in range(NV)]
            far = [part(z_halo, v) for v in range(NV)]
            a, b = face_terms(far, own, 2) if side == 0 else face_terms(own, far, 2)
            for v in range(NV):
                z_corr[side, v] = a[v] - b[v] if side == 0 else a[v] + b[v]

        def body(v, carry):
            for x in range(NX):
                res[v, x, 0:1, :] += y_corr[0, v, x : x + 1, :]
                res[v, x, NY - 1 : NY, :] += y_corr[1, v, x : x + 1, :]
                low = z_corr[0, v][:, x : x + 1]
                high = z_corr[1, v][:, x : x + 1]
                res[v, x, :, 0:LANES] += jnp.where(lane_1 == 0, low, 0.0)
                res[v, x, :, NZ - LANES : NZ] += jnp.where(lane_1 == LANES - 1, high, 0.0)
            return carry

        lax.fori_loop(0, NV, body, 0)

    def interior(sec):
        fluxes_and_jumps()
        if sec == 0:
            value = gather_top(0, tops_x, top_x)
            top[1] = value
            start(tops_z)
            loads[2].wait()
            loads[3].wait()
        lines_y_z()
        lines_x()
        y_z_faces(sec)

    def update(sec, x, c, extra):
        a, b = COEFFS[sec]
        rows = pl.ds(ROWS * c, ROWS)
        dt = step[...]
        for v in range(NV):
            r = res[v, x, rows, :]
            if extra is not None:
                r = r + extra[v]
            new_k = a * k[v, x, rows, :] + dt * r
            new_u = u[v, x, rows, :] + b * new_k
            if sec == 0:
                k[v, x, rows, :] = new_k
                u[v, x, rows, :] = new_u
            else:
                out_register[v, x, rows, :] = new_k
                out_state[v, x, rows, :] = new_u

    def update_boundary(sec, side, c):
        x_copy(sec, 1 - side, c).wait_recv()
        x = 0 if side == 0 else NX - 1
        own = chunk(u, x, c)
        far = [x_halo[sec, side, c, v] for v in range(NV)]
        a, b = face_terms(far, own, 0) if side == 0 else face_terms(own, far, 0)
        extra = [p - q if side == 0 else p + q for p, q in zip(a, b)]
        update(sec, x, c, extra)

    def update_interior(sec):
        def body(x, carry):
            for c in range(CH):
                update(sec, x, c, None)
            return carry

        lax.fori_loop(1, NX - 1, body, 0)

    pack(0)
    pl.semaphore_wait(barrier, len(partners))
    start(tops_x)
    start(y_z_copies(0))
    for c in range(CH):
        start([x_copy(0, 0, c), x_copy(0, 1, c)])

    interior(0)
    top[2] = gather_top(1, tops_z, top_z)
    start(tops_y)
    value = gather_top(2, tops_y, top_y)
    value = jnp.max(jnp.max(value, axis=0, keepdims=True), axis=1, keepdims=True)
    step[...] = jnp.broadcast_to(COURANT * ELEM_WIDTH / (11.0 * value), (ROWS, NZ))
    loads[1].wait()

    for c in range(CH):
        for side in (0, 1):
            update_boundary(0, side, c)
            if c == 0:
                x_copy(1, side, c).start()
    update_interior(0)
    pack(1)
    start(y_z_copies(1))
    for c in range(1, CH):
        start([x_copy(1, 0, c), x_copy(1, 1, c)])

    interior(1)
    update_interior(1)
    for c in range(CH):
        for side in (0, 1):
            update_boundary(1, side, c)

    for copy in tops_x + tops_z + tops_y:
        copy.wait_send()
    for sec in (0, 1):
        for copy in y_z_copies(sec):
            copy.wait_send()
        for c in range(CH):
            for side in (0, 1):
                x_copy(sec, side, c).wait_send()


def shards(sizes, state, register):
    mat_z, mat_y = operators()
    nz, nxl, ny, nxh, nco = sizes
    n_x, n_z, n_y = nxh * nxl * nco - 1, nz - 1, ny - 1
    block = (NV, NX, NY, NZ)
    vmem = lambda *shape: pltpu.VMEM(shape, jnp.float32)
    dma = lambda *shape: pltpu.SemaphoreType.DMA(shape)
    out = jax.ShapeDtypeStruct(block, jnp.float32)
    return pl.pallas_call(
        functools.partial(kernel, sizes),
        out_shape=(out, out),
        in_specs=[pl.BlockSpec(memory_space=pl.ANY)] * 4,
        out_specs=[pl.BlockSpec(memory_space=pltpu.VMEM)] * 2,
        scratch_shapes=[
            vmem(*block),
            vmem(*block),
            vmem(*block),
            vmem(*block),
            vmem(*block),
            vmem(*block),
            vmem(2, 2 * LANES, 2 * LANES),
            vmem(NX * NY, NX * NY),
            vmem(ROWS, NZ),
            vmem(ROWS, NZ),
            vmem(3, ROWS, LANES),
            vmem(n_x, ROWS, LANES),
            vmem(n_z, ROWS, LANES),
            vmem(n_y, ROWS, LANES),
            vmem(2, 2, NV, ROWS, NZ),
            vmem(2, 2, NY, LANES),
            vmem(2, 2, NV, ROWS, NZ),
            vmem(2, 2, NY, LANES),
            vmem(2, 2, CH, NV, ROWS, NZ),
            vmem(2, NV, ROWS, NZ),
            vmem(2, NV, NY, LANES),
            dma(4),
            dma(2, 2, CH),
            dma(2, 2, CH),
            dma(2, 2, 2),
            dma(2, 2, 2),
            dma(n_x + n_z + n_y),
            dma(n_x + n_z + n_y),
        ],
        compiler_params=pltpu.CompilerParams(
            collective_id=0, has_side_effects=True, vmem_limit_bytes=40 * 2**20
        ),
        name="sections",
    )(state, register, mat_z, mat_y)


def solution(mesh):
    gx, gy, gz = (mesh.shape[a] for a in ("gx", "gy", "gz"))
    sizes = (gx // 2, 2, gy, gz // 2, 2)
    torus = Mesh(mesh.devices.reshape(sizes), AXES)
    placed = P(None, ("gx_0", "gx_1"), "gy", ("gz_0", "gz_1"))
    return jax.shard_map(
        functools.partial(shards, sizes),
        mesh=torus,
        in_specs=(placed, placed),
        out_specs=(placed, placed),
        check_vma=False,
    )
```

```python
import functools
import math

import jax
import jax.numpy as jnp
import numpy as np
from jax import lax
from jax.experimental import pallas as pl
from jax.experimental.pallas import tpu as pltpu
from jax.sharding import Mesh
from jax.sharding import PartitionSpec as P

AXES = ("gx_0", "gx_1", "gy", "gz_0", "gz_1")
MESH = pl.DeviceIdType.MESH

GAMMA = 1.4
GM1 = 0.4
ELEM_WIDTH = 0.05
COURANT = 0.5
COEFFS = (
    (-567301805773.0 / 1357537059087.0, 5161836677717.0 / 13612068292357.0),
    (-2404267990393.0 / 2016746695238.0, 1720146321549.0 / 2090206949498.0),
)
NV = 5
N = 6
NX, NY, NZ = 6, 24, 384
ROWS = 8
CH = NY // ROWS
LANES = 128
SCALE = 2.0 / ELEM_WIDTH
FACE = SCALE * 15.0 * 0.5


def gll_derivative():
    seven = math.sqrt(7.0)
    inner = math.sqrt(1.0 / 3.0 - 2.0 * seven / 21.0)
    outer = math.sqrt(1.0 / 3.0 + 2.0 * seven / 21.0)
    points = np.array([-1.0, -outer, -inner, inner, outer, 1.0])
    count = len(points)
    weights = np.array(
        [np.prod([points[i] - points[j] for j in range(count) if j != i]) for i in range(count)]
    )
    table = np.zeros((count, count))
    for i in range(count):
        for j in range(count):
            if i != j:
                table[i, j] = weights[i] / weights[j] / (points[i] - points[j])
        table[i, i] = -np.sum(table[i])
    return table


DIFF = gll_derivative()


def line_operator(length):
    elems = length // N
    op = np.kron(np.eye(elems), -SCALE * DIFF)
    for e in range(elems - 1):
        last, first = N * e + N - 1, N * e + N
        for row in (last, first):
            op[row, last] += FACE
            op[row, first] -= FACE
    return op


def operators():
    along_z = line_operator(NZ).T
    cut = 2 * LANES - (2 * LANES) % N
    low = along_z[: 2 * LANES, : 2 * LANES].copy()
    low[:, cut:] = 0.0
    high = along_z[LANES:, LANES:].copy()
    high[:, : cut - LANES] = 0.0
    along_y = np.kron(np.eye(NX), line_operator(NY))
    return (
        jnp.asarray(np.stack([low, high]), jnp.float32),
        jnp.asarray(along_y, jnp.float32),
    )


def primitives(u):
    inv = 1.0 / u[0]
    vel = [u[1] * inv, u[2] * inv, u[3] * inv]
    press = GM1 * (u[4] - 0.5 * (u[1] * vel[0] + u[2] * vel[1] + u[3] * vel[2]))
    sound = jnp.sqrt(GAMMA * press * inv)
    return vel, press, sound


def flux(u, vel, press, d):
    parts = [u[1 + d], u[1] * vel[d], u[2] * vel[d], u[3] * vel[d], (u[4] + press) * vel[d]]
    parts[1 + d] = parts[1 + d] + press
    return parts


def face_terms(left, right, d):
    vel_l, press_l, sound_l = primitives(left)
    vel_r, press_r, sound_r = primitives(right)
    flux_l = flux(left, vel_l, press_l, d)
    flux_r = flux(right, vel_r, press_r, d)
    lam = FACE * jnp.maximum(jnp.abs(vel_l[d]) + sound_l, jnp.abs(vel_r[d]) + sound_r)
    a = [FACE * (fl - fr) for fl, fr in zip(flux_l, flux_r)]
    b = [lam * (r - l) for l, r in zip(left, right)]
    return a, b


def x_face(side, own, far):
    a, b = face_terms(far, own, 0) if side == 0 else face_terms(own, far, 0)
    return [p - q if side == 0 else p + q for p, q in zip(a, b)]


def advance(sec, k, u, dt, r):
    a, b = COEFFS[sec]
    new_k = a * k + dt * r
    return new_k, u + b * new_k


def kernel(
    sizes,
    state,
    register,
    mat_z,
    mat_y,
    u,
    k,
    edge,
    far_x,
    step,
    res,
    fx,
    fy,
    fz,
    mz,
    my,
    mask_z,
    top,
    top_x,
    top_z,
    top_y,
    y_pack,
    z_pack,
    y_halo,
    z_halo,
    near_x,
    y_corr,
    z_corr,
    load_sem,
    send_x,
    recv_x,
    send_yz,
    recv_yz,
    send_top,
    recv_top,
):
    nz, nxl, ny, nxh, nco = sizes
    z, xl, y, xh, co = (lax.axis_index(a) for a in AXES)

    def device(z_=z, xl_=xl, y_=y, xh_=xh, co_=co):
        return dict(zip(AXES, (z_, xl_, y_, xh_, co_)))

    def wrap(i, n):
        return lax.rem(i + n, n)

    other_xl, other_co = wrap(xl + 1, nxl), wrap(co + 1, nco)
    gx = (
        device(z_=wrap(z + xl - 1, nz), xl_=other_xl),
        device(z_=wrap(z + xl, nz), xl_=other_xl),
    )
    gy = (device(y_=wrap(y - 1, ny)), device(y_=wrap(y + 1, ny)))
    gz = (
        device(xh_=wrap(xh + co - 1, nxh), co_=other_co),
        device(xh_=wrap(xh + co, nxh), co_=other_co),
    )
    group_x = [
        device(xh_=wrap(xh + a, nxh), xl_=wrap(xl + b, nxl), co_=wrap(co + c, nco))
        for a in range(nxh)
        for b in range(nxl)
        for c in range(nco)
        if a or b or c
    ]
    group_z = [device(z_=wrap(z + i, nz)) for i in range(1, nz)]
    group_y = [device(y_=wrap(y + i, ny)) for i in range(1, ny)]
    diagonal = device(z_=wrap(z + 2 * xl - 1, nz), xl_=other_xl)

    loads = [
        pltpu.make_async_copy(state, u, load_sem.at[0]),
        pltpu.make_async_copy(register, k, load_sem.at[1]),
        pltpu.make_async_copy(mat_z, mz, load_sem.at[2]),
        pltpu.make_async_copy(mat_y, my, load_sem.at[3]),
    ]
    for load in loads:
        load.start()
    barrier = pltpu.get_barrier_semaphore()
    partners = group_x + group_z + group_y + [diagonal]
    for partner in partners:
        pl.semaphore_signal(barrier, inc=1, device_id=partner, device_id_type=MESH)

    lane = lax.broadcasted_iota(jnp.int32, (ROWS, NZ), 1)
    lane_f = lane.astype(jnp.float32)
    place = lane_f - N * jnp.floor((lane_f + 0.5) * (1.0 / N))
    mask_z[...] = jnp.where((place > N - 1.5) & (lane < NZ - 1), FACE, 0.0)
    row = lax.broadcasted_iota(jnp.int32, (ROWS, NZ), 0)
    lane_1 = lax.broadcasted_iota(jnp.int32, (NY, LANES), 1)

    def chunk(ref, x, c):
        return [ref[v, x, pl.ds(ROWS * c, ROWS), :] for v in range(NV)]

    loads[0].wait()
    top[0] = jnp.zeros((ROWS, LANES), jnp.float32)

    def speed_body(x, carry):
        for c in range(CH):
            w = chunk(u, x, c)
            vel, press, sound = primitives(w)
            mom = jnp.sqrt(w[1] * w[1] + w[2] * w[2] + w[3] * w[3])
            s = mom * (1.0 / w[0]) + sound
            carry = jnp.maximum(carry, s)
        return carry

    best = lax.fori_loop(0, NX, speed_body, jnp.zeros((ROWS, NZ), jnp.float32))
    top[0] = jnp.maximum(
        jnp.maximum(best[:, :LANES], best[:, LANES : 2 * LANES]), best[:, 2 * LANES :]
    )

    def pack(sec):
        def body(v, carry):
            low, high = carry
            for x in range(NX):
                y_pack[sec, 0, v, x : x + 1, :] = u[v, x, 0:1, :]
                y_pack[sec, 1, v, x : x + 1, :] = u[v, x, NY - 1 : NY, :]
                here = lane_1 == v * NX + x
                low = jnp.where(here, u[v, x, :, 0:LANES][:, 0:1], low)
                high = jnp.where(here, u[v, x, :, NZ - LANES : NZ][:, LANES - 1 : LANES], high)
            for x in range(NX, ROWS):
                y_pack[sec, 0, v, x : x + 1, :] = u[v, 0, 0:1, :]
                y_pack[sec, 1, v, x : x + 1, :] = u[v, 0, NY - 1 : NY, :]
            return low, high

        ones = jnp.ones((NY, LANES), jnp.float32)
        low, high = lax.fori_loop(0, NV, body, (ones, ones))
        z_pack[sec, 0] = low
        z_pack[sec, 1] = high

    def remote(src, dst, send, recv, to):
        return pltpu.make_async_remote_copy(
            src_ref=src,
            dst_ref=dst,
            send_sem=send,
            recv_sem=recv,
            device_id=to,
            device_id_type=MESH,
        )

    def x_copy(sec, side, c):
        src = state if sec == 0 else u
        return remote(
            src.at[:, 0 if side == 0 else NX - 1, pl.ds(ROWS * c, ROWS), :],
            (far_x if sec else near_x).at[1 - side, c],
            send_x.at[sec, side, c],
            recv_x.at[sec, 1 - side, c],
            gx[side],
        )

    def y_copy(sec, side):
        return remote(
            y_pack.at[sec, side],
            y_halo.at[sec, 1 - side],
            send_yz.at[sec, 0, side],
            recv_yz.at[sec, 0, 1 - side],
            gy[side],
        )

    def z_copy(sec, side):
        return remote(
            z_pack.at[sec, side],
            z_halo.at[sec, 1 - side],
            send_yz.at[sec, 1, side],
            recv_yz.at[sec, 1, 1 - side],
            gz[side],
        )

    def top_copies(stage, group, slots, first):
        return [
            remote(top.at[stage], slots.at[i], send_top.at[first + i], recv_top.at[first + i], to)
            for i, to in enumerate(group)
        ]

    tops_x = top_copies(0, group_x, top_x, 0)
    tops_z = top_copies(1, group_z, top_z, len(group_x))
    tops_y = top_copies(2, group_y, top_y, len(group_x) + len(group_z))

    def start(copies):
        for copy in copies:
            copy.start()

    def gather_top(stage, copies, slots):
        value = top[stage]
        for i, copy in enumerate(copies):
            copy.wait_recv()
            value = jnp.maximum(value, slots[i])
        return value

    def y_z_copies(sec):
        return [z_copy(sec, 0), z_copy(sec, 1), y_copy(sec, 0), y_copy(sec, 1)]

    def fluxes_and_jumps():
        def body(x, carry):
            for c in range(CH):
                w = chunk(u, x, c)
                vel, press, sound = primitives(w)
                rows = pl.ds(ROWS * c, ROWS)
                for d, to in enumerate((fx, fy, fz)):
                    for v, part in enumerate(flux(w, vel, press, d)):
                        to[v, x, rows, :] = part
                s_y = jnp.abs(vel[1]) + sound
                s_z = jnp.abs(vel[2]) + sound
                lam_y = jnp.where(
                    row == N - 1 - 2 * c,
                    FACE * jnp.maximum(s_y, pltpu.roll(s_y, ROWS - 1, 0)),
                    0.0,
                )
                lam_z = mask_z[...] * jnp.maximum(s_z, pltpu.roll(s_z, NZ - 1, 1))
                for v in range(NV):
                    t_y = lam_y * (pltpu.roll(w[v], ROWS - 1, 0) - w[v])
                    t_z = lam_z * (pltpu.roll(w[v], NZ - 1, 1) - w[v])
                    res[v, x, rows, :] = (t_y - pltpu.roll(t_y, 1, 0)) + (
                        t_z - pltpu.roll(t_z, 1, 1)
                    )
            return carry

        lax.fori_loop(0, NX, body, 0)

    def dot(a, b):
        return jnp.dot(
            a, b, precision=lax.Precision.HIGHEST, preferred_element_type=jnp.float32
        )

    def lines_y_z():
        def body(v, carry):
            along_z = fz[v].reshape(NX * NY, NZ)
            low = dot(along_z[:, : 2 * LANES], mz[0])
            high = dot(along_z[:, LANES:], mz[1])
            both = jnp.concatenate(
                [low[:, :LANES], low[:, LANES:] + high[:, :LANES], high[:, LANES:]], axis=1
            )
            along_y = dot(my[...], fy[v].reshape(NX * NY, NZ))
            res[v] = res[v] + (both + along_y).reshape(NX, NY, NZ)
            return carry

        lax.fori_loop(0, NV, body, 0)

    def lines_x():
        half = N // 2
        even = [[-SCALE * 0.5 * (DIFF[i, j] + DIFF[i, N - 1 - j]) for j in range(half)] for i in range(half)]
        odd = [[-SCALE * 0.5 * (DIFF[i, j] - DIFF[i, N - 1 - j]) for j in range(half)] for i in range(half)]

        def body(v, carry):
            for c in range(CH):
                rows = pl.ds(ROWS * c, ROWS)
                f = [fx[v, x, rows, :] for x in range(NX)]
                plus = [f[j] + f[N - 1 - j] for j in range(half)]
                minus = [f[j] - f[N - 1 - j] for j in range(half)]
                for i in range(half):
                    a = sum(even[i][j] * plus[j] for j in range(half))
                    b = sum(odd[i][j] * minus[j] for j in range(half))
                    res[v, i, rows, :] += b + a
                    res[v, N - 1 - i, rows, :] += b - a
            return carry

        lax.fori_loop(0, NV, body, 0)

    def y_z_faces(sec):
        for side in (0, 1):
            y_copy(sec, 1 - side).wait_recv()
            own = [y_pack[sec, side, v] for v in range(NV)]
            far = [y_halo[sec, side, v] for v in range(NV)]
            a, b = face_terms(far, own, 1) if side == 0 else face_terms(own, far, 1)
            for v in range(NV):
                y_corr[side, v] = a[v] - b[v] if side == 0 else a[v] + b[v]
            z_copy(sec, 1 - side).wait_recv()

            def part(ref, v):
                tile = ref[sec, side]
                return tile if v == 0 else pltpu.roll(tile, LANES - NX * v, 1)

            own = [part(z_pack, v) for v in range(NV)]
            far = [part(z_halo, v) for v in range(NV)]
            a, b = face_terms(far, own, 2) if side == 0 else face_terms(own, far, 2)
            for v in range(NV):
                z_corr[side, v] = a[v] - b[v] if side == 0 else a[v] + b[v]

        def body(v, carry):
            for x in range(NX):
                res[v, x, 0:1, :] += y_corr[0, v, x : x + 1, :]
                res[v, x, NY - 1 : NY, :] += y_corr[1, v, x : x + 1, :]
                low = z_corr[0, v][:, x : x + 1]
                high = z_corr[1, v][:, x : x + 1]
                res[v, x, :, 0:LANES] += jnp.where(lane_1 == 0, low, 0.0)
                res[v, x, :, NZ - LANES : NZ] += jnp.where(lane_1 == LANES - 1, high, 0.0)
            return carry

        lax.fori_loop(0, NV, body, 0)

    def interior(sec):
        fluxes_and_jumps()
        if sec == 0:
            value = gather_top(0, tops_x, top_x)
            top[1] = value
            start(tops_z)
            loads[2].wait()
            loads[3].wait()
        lines_y_z()
        lines_x()

    def update(sec, x, c, extra):
        rows = pl.ds(ROWS * c, ROWS)
        for v in range(NV):
            r = res[v, x, rows, :]
            if extra is not None:
                r = r + extra[v]
            new_k, new_u = advance(sec, k[v, x, rows, :], u[v, x, rows, :], step[...], r)
            k[v, x, rows, :] = new_k
            u[v, x, rows, :] = new_u

    def update_boundary(side, c):
        x_copy(0, 1 - side, c).wait_recv()
        x = 0 if side == 0 else NX - 1
        own = chunk(u, x, c)
        far = [near_x[side, c, v] for v in range(NV)]
        update(0, x, c, x_face(side, own, far))

    def update_interior(sec):
        def body(x, carry):
            for c in range(CH):
                update(sec, x, c, None)
            return carry

        lax.fori_loop(1, NX - 1, body, 0)

    pl.semaphore_wait(barrier, len(partners))
    start(tops_x)
    pack(0)
    start(y_z_copies(0))
    for c in range(CH):
        start([x_copy(0, 0, c), x_copy(0, 1, c)])

    interior(0)
    top[2] = gather_top(1, tops_z, top_z)
    start(tops_y)
    y_z_faces(0)
    value = gather_top(2, tops_y, top_y)
    value = jnp.max(jnp.max(value, axis=0, keepdims=True), axis=1, keepdims=True)
    step[...] = jnp.broadcast_to(COURANT * ELEM_WIDTH / (11.0 * value), (ROWS, NZ))
    loads[1].wait()

    for c in range(CH):
        for side in (0, 1):
            update_boundary(side, c)
            if c == 0:
                x_copy(1, side, c).start()
    update_interior(0)
    pack(1)
    start(y_z_copies(1))
    for c in range(1, CH):
        start([x_copy(1, 0, c), x_copy(1, 1, c)])

    interior(1)
    y_z_faces(1)
    update_interior(1)
    for v in range(NV):
        edge[0, v] = res[v, 0]
        edge[1, v] = res[v, NX - 1]
    for c in range(CH):
        for side in (0, 1):
            x_copy(1, side, c).wait_recv()

    for copy in tops_x + tops_z + tops_y:
        copy.wait_send()
    for sec in (0, 1):
        for copy in y_z_copies(sec):
            copy.wait_send()
        for c in range(CH):
            for side in (0, 1):
                x_copy(sec, side, c).wait_send()


def finish(u, k, edge, far_x, step, out_state, out_register, done, sem):
    inner = [
        pltpu.make_async_copy(
            src.at[:, pl.ds(1, NX - 2)], dst.at[:, pl.ds(1, NX - 2)], sem.at[i, 0]
        )
        for i, (src, dst) in enumerate(((u, out_state), (k, out_register)))
    ]
    for copy in inner:
        copy.start()
    outer = []
    for side in (0, 1):
        x = 0 if side == 0 else NX - 1
        for c in range(CH):
            rows = pl.ds(ROWS * c, ROWS)
            own = [u[v, x, rows, :] for v in range(NV)]
            far = [far_x[side, c, v] for v in range(NV)]
            extra = x_face(side, own, far)
            for v in range(NV):
                new_k, new_u = advance(
                    1, k[v, x, rows, :], own[v], step[...], edge[side, v, rows, :] + extra[v]
                )
                done[0, side, v, rows, :] = new_u
                done[1, side, v, rows, :] = new_k
        for i, dst in enumerate((out_state, out_register)):
            copy = pltpu.make_async_copy(done.at[i, side], dst.at[:, x], sem.at[i, 1 + side])
            copy.start()
            outer.append(copy)
    for copy in inner + outer:
        copy.wait()


def shards(sizes, state, register):
    mat_z, mat_y = operators()
    nz, nxl, ny, nxh, nco = sizes
    n_x, n_z, n_y = nxh * nxl * nco - 1, nz - 1, ny - 1
    block = (NV, NX, NY, NZ)
    vmem = lambda *shape: pltpu.VMEM(shape, jnp.float32)
    dma = lambda *shape: pltpu.SemaphoreType.DMA(shape)
    array = lambda *shape: jax.ShapeDtypeStruct(shape, jnp.float32)
    in_vmem = pl.BlockSpec(memory_space=pltpu.VMEM)
    in_hbm = pl.BlockSpec(memory_space=pltpu.HBM)
    parts = pl.pallas_call(
        functools.partial(kernel, sizes),
        out_shape=(
            array(*block),
            array(*block),
            array(2, NV, NY, NZ),
            array(2, CH, NV, ROWS, NZ),
            array(ROWS, NZ),
        ),
        in_specs=[in_hbm] * 4,
        out_specs=[in_vmem] * 5,
        scratch_shapes=[
            vmem(*block),
            vmem(*block),
            vmem(*block),
            vmem(*block),
            vmem(2, 2 * LANES, 2 * LANES),
            vmem(NX * NY, NX * NY),
            vmem(ROWS, NZ),
            vmem(3, ROWS, LANES),
            vmem(n_x, ROWS, LANES),
            vmem(n_z, ROWS, LANES),
            vmem(n_y, ROWS, LANES),
            vmem(2, 2, NV, ROWS, NZ),
            vmem(2, 2, NY, LANES),
            vmem(2, 2, NV, ROWS, NZ),
            vmem(2, 2, NY, LANES),
            vmem(2, CH, NV, ROWS, NZ),
            vmem(2, NV, ROWS, NZ),
            vmem(2, NV, NY, LANES),
            dma(4),
            dma(2, 2, CH),
            dma(2, 2, CH),
            dma(2, 2, 2),
            dma(2, 2, 2),
            dma(n_x + n_z + n_y),
            dma(n_x + n_z + n_y),
        ],
        compiler_params=pltpu.CompilerParams(
            collective_id=0, has_side_effects=True, vmem_limit_bytes=32 * 2**20
        ),
        name="sections",
    )(*[pltpu.with_memory_space_constraint(x, pltpu.HBM) for x in (state, register, mat_z, mat_y)])
    return pl.pallas_call(
        finish,
        out_shape=(array(*block), array(*block)),
        in_specs=[in_vmem] * 5,
        out_specs=[in_hbm] * 2,
        scratch_shapes=[vmem(2, 2, NV, NY, NZ), dma(2, 3)],
        compiler_params=pltpu.CompilerParams(vmem_limit_bytes=16 * 2**20),
        name="finish",
    )(*parts)


def solution(mesh):
    gx, gy, gz = (mesh.shape[a] for a in ("gx", "gy", "gz"))
    sizes = (gx // 2, 2, gy, gz // 2, 2)
    torus = Mesh(mesh.devices.reshape(sizes), AXES)
    placed = P(None, ("gx_0", "gx_1"), "gy", ("gz_0", "gz_1"))
    return jax.shard_map(
        functools.partial(shards, sizes),
        mesh=torus,
        in_specs=(placed, placed),
        out_specs=(placed, placed),
        check_vma=False,
    )
```

```python
import functools
import math

import jax
import jax.numpy as jnp
import numpy as np
from jax import lax
from jax.experimental import pallas as pl
from jax.experimental.pallas import tpu as pltpu
from jax.sharding import Mesh
from jax.sharding import PartitionSpec as P

AXES = ("gx_0", "gx_1", "gy", "gz_0", "gz_1")
MESH = pl.DeviceIdType.MESH

GAMMA = 1.4
GM1 = 0.4
ELEM_WIDTH = 0.05
COURANT = 0.5
COEFFS = (
    (-567301805773.0 / 1357537059087.0, 5161836677717.0 / 13612068292357.0),
    (-2404267990393.0 / 2016746695238.0, 1720146321549.0 / 2090206949498.0),
)
NV = 5
N = 6
NX, NY, NZ = 6, 24, 384
ROWS = 8
CH = NY // ROWS
LANES = 128
SCALE = 2.0 / ELEM_WIDTH
FACE = SCALE * 15.0 * 0.5


def gll_derivative():
    seven = math.sqrt(7.0)
    inner = math.sqrt(1.0 / 3.0 - 2.0 * seven / 21.0)
    outer = math.sqrt(1.0 / 3.0 + 2.0 * seven / 21.0)
    points = np.array([-1.0, -outer, -inner, inner, outer, 1.0])
    count = len(points)
    weights = np.array(
        [np.prod([points[i] - points[j] for j in range(count) if j != i]) for i in range(count)]
    )
    table = np.zeros((count, count))
    for i in range(count):
        for j in range(count):
            if i != j:
                table[i, j] = weights[i] / weights[j] / (points[i] - points[j])
        table[i, i] = -np.sum(table[i])
    return table


DIFF = gll_derivative()


def line_operator(length):
    elems = length // N
    op = np.kron(np.eye(elems), -SCALE * DIFF)
    for e in range(elems - 1):
        last, first = N * e + N - 1, N * e + N
        for row in (last, first):
            op[row, last] += FACE
            op[row, first] -= FACE
    return op


def operators():
    along_z = line_operator(NZ).T
    cut = 2 * LANES - (2 * LANES) % N
    low = along_z[: 2 * LANES, : 2 * LANES].copy()
    low[:, cut:] = 0.0
    high = along_z[LANES:, LANES:].copy()
    high[:, : cut - LANES] = 0.0
    along_y = np.kron(np.eye(NX), line_operator(NY))
    return (
        jnp.asarray(np.stack([low, high]), jnp.float32),
        jnp.asarray(along_y, jnp.float32),
    )


def primitives(u):
    inv = 1.0 / u[0]
    vel = [u[1] * inv, u[2] * inv, u[3] * inv]
    press = GM1 * (u[4] - 0.5 * (u[1] * vel[0] + u[2] * vel[1] + u[3] * vel[2]))
    sound = jnp.sqrt(GAMMA * press * inv)
    return vel, press, sound


def flux(u, vel, press, d):
    parts = [u[1 + d], u[1] * vel[d], u[2] * vel[d], u[3] * vel[d], (u[4] + press) * vel[d]]
    parts[1 + d] = parts[1 + d] + press
    return parts


def face_terms(left, right, d):
    vel_l, press_l, sound_l = primitives(left)
    vel_r, press_r, sound_r = primitives(right)
    flux_l = flux(left, vel_l, press_l, d)
    flux_r = flux(right, vel_r, press_r, d)
    lam = FACE * jnp.maximum(jnp.abs(vel_l[d]) + sound_l, jnp.abs(vel_r[d]) + sound_r)
    a = [FACE * (fl - fr) for fl, fr in zip(flux_l, flux_r)]
    b = [lam * (r - l) for l, r in zip(left, right)]
    return a, b


def x_face(side, own, far):
    a, b = face_terms(far, own, 0) if side == 0 else face_terms(own, far, 0)
    return [p - q if side == 0 else p + q for p, q in zip(a, b)]


def advance(sec, k, u, dt, r):
    a, b = COEFFS[sec]
    new_k = a * k + dt * r
    return new_k, u + b * new_k


def kernel(
    sizes,
    state,
    register,
    mat_z,
    mat_y,
    u,
    k,
    edge,
    far_x,
    step,
    res,
    fx,
    fy,
    fz,
    mz,
    my,
    mask_z,
    top,
    top_far,
    top_near,
    y_pack,
    z_pack,
    y_halo,
    z_halo,
    near_x,
    y_corr,
    z_corr,
    load_sem,
    send_x,
    recv_x,
    send_yz,
    recv_yz,
    send_top,
    recv_top,
):
    nz, nxl, ny, nxh, nco = sizes
    z, xl, y, xh, co = (lax.axis_index(a) for a in AXES)

    def device(z_=z, xl_=xl, y_=y, xh_=xh, co_=co):
        return dict(zip(AXES, (z_, xl_, y_, xh_, co_)))

    def wrap(i, n):
        return lax.rem(i + n, n)

    other_xl, other_co = wrap(xl + 1, nxl), wrap(co + 1, nco)
    gx = (
        device(z_=wrap(z + xl - 1, nz), xl_=other_xl),
        device(z_=wrap(z + xl, nz), xl_=other_xl),
    )
    gy = (device(y_=wrap(y - 1, ny)), device(y_=wrap(y + 1, ny)))
    gz = (
        device(xh_=wrap(xh + co - 1, nxh), co_=other_co),
        device(xh_=wrap(xh + co, nxh), co_=other_co),
    )
    far = [
        (min(i, nz - i) + (2 * a if a != b else 1 if b else 0), i, a, b)
        for i in range(nz)
        for a in range(nxh)
        for b in range(nxl)
        if i or a or b
    ]
    group_far = [
        device(z_=wrap(z + i, nz), xh_=wrap(xh + a, nxh), xl_=wrap(xl + b, nxl))
        for _, i, a, b in sorted(far, reverse=True)
    ]
    group_near = [
        device(y_=wrap(y + i, ny), co_=wrap(co + c, nco))
        for i in range(ny)
        for c in range(nco)
        if i or c
    ]
    across = [device(xh_=wrap(xh + 1, nxh), co_=other_co)]

    loads = [
        pltpu.make_async_copy(mat_z, mz, load_sem.at[NX]),
        pltpu.make_async_copy(mat_y, my, load_sem.at[NX + 1]),
        pltpu.make_async_copy(register, k, load_sem.at[NX + 2]),
    ]

    def load_plane(x):
        return pltpu.make_async_copy(state.at[:, x], u.at[:, x], load_sem.at[x])

    for x in range(NX):
        load_plane(x).start()
    for load in loads:
        load.start()
    barrier = pltpu.get_barrier_semaphore()
    partners = group_far + group_near + across[: nxh - 1]
    for partner in partners:
        pl.semaphore_signal(barrier, inc=1, device_id=partner, device_id_type=MESH)

    lane = lax.broadcasted_iota(jnp.int32, (ROWS, NZ), 1)
    lane_f = lane.astype(jnp.float32)
    place = lane_f - N * jnp.floor((lane_f + 0.5) * (1.0 / N))
    mask_z[...] = jnp.where((place > N - 1.5) & (lane < NZ - 1), FACE, 0.0)
    row = lax.broadcasted_iota(jnp.int32, (ROWS, NZ), 0)
    lane_1 = lax.broadcasted_iota(jnp.int32, (NY, LANES), 1)

    def chunk(ref, x, c):
        return [ref[v, x, pl.ds(ROWS * c, ROWS), :] for v in range(NV)]

    def speed_body(x, carry):
        load_plane(x).wait()
        for c in range(CH):
            w = chunk(u, x, c)
            vel, press, sound = primitives(w)
            mom = jnp.sqrt(w[1] * w[1] + w[2] * w[2] + w[3] * w[3])
            s = mom * (1.0 / w[0]) + sound
            carry = jnp.maximum(carry, s)
        return carry

    best = lax.fori_loop(0, NX, speed_body, jnp.zeros((ROWS, NZ), jnp.float32))
    best = jnp.maximum(
        jnp.maximum(best[:, :LANES], best[:, LANES : 2 * LANES]), best[:, 2 * LANES :]
    )
    top[0] = jnp.max(best, axis=0, keepdims=True)

    def pack(sec):
        def body(v, carry):
            low, high = carry
            for x in range(NX):
                y_pack[sec, 0, v, x : x + 1, :] = u[v, x, 0:1, :]
                y_pack[sec, 1, v, x : x + 1, :] = u[v, x, NY - 1 : NY, :]
                here = lane_1 == v * NX + x
                low = jnp.where(here, u[v, x, :, 0:LANES][:, 0:1], low)
                high = jnp.where(here, u[v, x, :, NZ - LANES : NZ][:, LANES - 1 : LANES], high)
            for x in range(NX, ROWS):
                y_pack[sec, 0, v, x : x + 1, :] = u[v, 0, 0:1, :]
                y_pack[sec, 1, v, x : x + 1, :] = u[v, 0, NY - 1 : NY, :]
            return low, high

        ones = jnp.ones((NY, LANES), jnp.float32)
        low, high = lax.fori_loop(0, NV, body, (ones, ones))
        z_pack[sec, 0] = low
        z_pack[sec, 1] = high

    def remote(src, dst, send, recv, to):
        return pltpu.make_async_remote_copy(
            src_ref=src,
            dst_ref=dst,
            send_sem=send,
            recv_sem=recv,
            device_id=to,
            device_id_type=MESH,
        )

    def x_copy(sec, side, c):
        src = state if sec == 0 else u
        return remote(
            src.at[:, 0 if side == 0 else NX - 1, pl.ds(ROWS * c, ROWS), :],
            (far_x if sec else near_x).at[1 - side, c],
            send_x.at[sec, side, c],
            recv_x.at[sec, 1 - side, c],
            gx[side],
        )

    def y_copy(sec, side):
        return remote(
            y_pack.at[sec, side],
            y_halo.at[sec, 1 - side],
            send_yz.at[sec, 0, side],
            recv_yz.at[sec, 0, 1 - side],
            gy[side],
        )

    def z_copy(sec, side):
        return remote(
            z_pack.at[sec, side],
            z_halo.at[sec, 1 - side],
            send_yz.at[sec, 1, side],
            recv_yz.at[sec, 1, 1 - side],
            gz[side],
        )

    def top_copies(stage, group, slots, first):
        return [
            remote(top.at[stage], slots.at[i], send_top.at[first + i], recv_top.at[first + i], to)
            for i, to in enumerate(group)
        ]

    tops_far = top_copies(0, group_far, top_far, 0)
    tops_near = top_copies(1, group_near, top_near, len(group_far))

    def start(copies):
        for copy in copies:
            copy.start()

    def gather_top(stage, copies, slots):
        value = top[stage]
        for i, copy in enumerate(copies):
            copy.wait_recv()
            value = jnp.maximum(value, slots[i])
        return value

    def y_z_copies(sec):
        return [z_copy(sec, 0), z_copy(sec, 1), y_copy(sec, 0), y_copy(sec, 1)]

    def fluxes_and_jumps():
        def body(x, carry):
            for c in range(CH):
                w = chunk(u, x, c)
                vel, press, sound = primitives(w)
                rows = pl.ds(ROWS * c, ROWS)
                for d, to in enumerate((fx, fy, fz)):
                    for v, part in enumerate(flux(w, vel, press, d)):
                        to[v, x, rows, :] = part
                s_y = jnp.abs(vel[1]) + sound
                s_z = jnp.abs(vel[2]) + sound
                lam_y = jnp.where(
                    row == N - 1 - 2 * c,
                    FACE * jnp.maximum(s_y, pltpu.roll(s_y, ROWS - 1, 0)),
                    0.0,
                )
                lam_z = mask_z[...] * jnp.maximum(s_z, pltpu.roll(s_z, NZ - 1, 1))
                for v in range(NV):
                    t_y = lam_y * (pltpu.roll(w[v], ROWS - 1, 0) - w[v])
                    t_z = lam_z * (pltpu.roll(w[v], NZ - 1, 1) - w[v])
                    res[v, x, rows, :] = (t_y - pltpu.roll(t_y, 1, 0)) + (
                        t_z - pltpu.roll(t_z, 1, 1)
                    )
            return carry

        lax.fori_loop(0, NX, body, 0)

    def dot(a, b):
        return jnp.dot(
            a, b, precision=lax.Precision.HIGHEST, preferred_element_type=jnp.float32
        )

    def lines_y_z():
        def body(v, carry):
            along_z = fz[v].reshape(NX * NY, NZ)
            low = dot(along_z[:, : 2 * LANES], mz[0])
            high = dot(along_z[:, LANES:], mz[1])
            both = jnp.concatenate(
                [low[:, :LANES], low[:, LANES:] + high[:, :LANES], high[:, LANES:]], axis=1
            )
            along_y = dot(my[...], fy[v].reshape(NX * NY, NZ))
            res[v] = res[v] + (both + along_y).reshape(NX, NY, NZ)
            return carry

        lax.fori_loop(0, NV, body, 0)

    def lines_x():
        half = N // 2
        even = [[-SCALE * 0.5 * (DIFF[i, j] + DIFF[i, N - 1 - j]) for j in range(half)] for i in range(half)]
        odd = [[-SCALE * 0.5 * (DIFF[i, j] - DIFF[i, N - 1 - j]) for j in range(half)] for i in range(half)]

        def body(v, carry):
            for c in range(CH):
                rows = pl.ds(ROWS * c, ROWS)
                f = [fx[v, x, rows, :] for x in range(NX)]
                plus = [f[j] + f[N - 1 - j] for j in range(half)]
                minus = [f[j] - f[N - 1 - j] for j in range(half)]
                for i in range(half):
                    a = sum(even[i][j] * plus[j] for j in range(half))
                    b = sum(odd[i][j] * minus[j] for j in range(half))
                    res[v, i, rows, :] += b + a
                    res[v, N - 1 - i, rows, :] += b - a
            return carry

        lax.fori_loop(0, NV, body, 0)

    def y_z_faces(sec):
        for side in (0, 1):
            y_copy(sec, 1 - side).wait_recv()
            own = [y_pack[sec, side, v] for v in range(NV)]
            far = [y_halo[sec, side, v] for v in range(NV)]
            a, b = face_terms(far, own, 1) if side == 0 else face_terms(own, far, 1)
            for v in range(NV):
                y_corr[side, v] = a[v] - b[v] if side == 0 else a[v] + b[v]
            z_copy(sec, 1 - side).wait_recv()

            def part(ref, v):
                tile = ref[sec, side]
                return tile if v == 0 else pltpu.roll(tile, LANES - NX * v, 1)

            own = [part(z_pack, v) for v in range(NV)]
            far = [part(z_halo, v) for v in range(NV)]
            a, b = face_terms(far, own, 2) if side == 0 else face_terms(own, far, 2)
            for v in range(NV):
                z_corr[side, v] = a[v] - b[v] if side == 0 else a[v] + b[v]

        def body(v, carry):
            for x in range(NX):
                res[v, x, 0:1, :] += y_corr[0, v, x : x + 1, :]
                res[v, x, NY - 1 : NY, :] += y_corr[1, v, x : x + 1, :]
                low = z_corr[0, v][:, x : x + 1]
                high = z_corr[1, v][:, x : x + 1]
                res[v, x, :, 0:LANES] += jnp.where(lane_1 == 0, low, 0.0)
                res[v, x, :, NZ - LANES : NZ] += jnp.where(lane_1 == LANES - 1, high, 0.0)
            return carry

        lax.fori_loop(0, NV, body, 0)

    def interior(sec):
        fluxes_and_jumps()
        if sec == 0:
            loads[0].wait()
            loads[1].wait()
            top[1] = gather_top(0, tops_far, top_far)
            start(tops_near)
        lines_y_z()
        lines_x()

    def update(sec, x, c, extra):
        rows = pl.ds(ROWS * c, ROWS)
        for v in range(NV):
            r = res[v, x, rows, :]
            if extra is not None:
                r = r + extra[v]
            new_k, new_u = advance(sec, k[v, x, rows, :], u[v, x, rows, :], step[...], r)
            k[v, x, rows, :] = new_k
            u[v, x, rows, :] = new_u

    def update_boundary(side, c):
        x_copy(0, 1 - side, c).wait_recv()
        x = 0 if side == 0 else NX - 1
        own = chunk(u, x, c)
        far = [near_x[side, c, v] for v in range(NV)]
        update(0, x, c, x_face(side, own, far))

    def update_interior(sec):
        def body(x, carry):
            for c in range(CH):
                update(sec, x, c, None)
            return carry

        lax.fori_loop(1, NX - 1, body, 0)

    pl.semaphore_wait(barrier, len(partners))
    start(tops_far)
    start([x_copy(0, 0, 0), x_copy(0, 1, 0)])
    pack(0)
    start(y_z_copies(0))
    for c in range(1, CH):
        start([x_copy(0, 0, c), x_copy(0, 1, c)])

    interior(0)
    y_z_faces(0)
    value = gather_top(1, tops_near, top_near)
    value = jnp.max(jnp.broadcast_to(value, (ROWS, LANES)), axis=1, keepdims=True)
    step[...] = jnp.broadcast_to(COURANT * ELEM_WIDTH / (11.0 * value), (ROWS, NZ))
    loads[2].wait()

    for c in range(CH):
        for side in (0, 1):
            update_boundary(side, c)
            if c < CH - 1:
                x_copy(1, side, c).start()
    update_interior(0)
    pack(1)
    start(y_z_copies(1))
    start([x_copy(1, 0, CH - 1), x_copy(1, 1, CH - 1)])

    interior(1)
    y_z_faces(1)
    update_interior(1)
    for v in range(NV):
        edge[0, v] = res[v, 0]
        edge[1, v] = res[v, NX - 1]
    for c in range(CH):
        for side in (0, 1):
            x_copy(1, side, c).wait_recv()

    for copy in tops_far + tops_near:
        copy.wait_send()
    for sec in (0, 1):
        for copy in y_z_copies(sec):
            copy.wait_send()
        for c in range(CH):
            for side in (0, 1):
                x_copy(sec, side, c).wait_send()


def finish(u, k, edge, far_x, step, out_state, out_register, done, sem):
    inner = [
        pltpu.make_async_copy(
            src.at[:, pl.ds(1, NX - 2)], dst.at[:, pl.ds(1, NX - 2)], sem.at[i, 0]
        )
        for i, (src, dst) in enumerate(((u, out_state), (k, out_register)))
    ]
    for copy in inner:
        copy.start()
    outer = []
    for side in (0, 1):
        x = 0 if side == 0 else NX - 1
        for c in range(CH):
            rows = pl.ds(ROWS * c, ROWS)
            own = [u[v, x, rows, :] for v in range(NV)]
            far = [far_x[side, c, v] for v in range(NV)]
            extra = x_face(side, own, far)
            for v in range(NV):
                new_k, new_u = advance(
                    1, k[v, x, rows, :], own[v], step[...], edge[side, v, rows, :] + extra[v]
                )
                done[0, side, v, rows, :] = new_u
                done[1, side, v, rows, :] = new_k
        for i, dst in enumerate((out_state, out_register)):
            copy = pltpu.make_async_copy(done.at[i, side], dst.at[:, x], sem.at[i, 1 + side])
            copy.start()
            outer.append(copy)
    for copy in inner + outer:
        copy.wait()


def shards(sizes, state, register):
    mat_z, mat_y = operators()
    nz, nxl, ny, nxh, nco = sizes
    n_far, n_near = nz * nxh * nxl - 1, ny * nco - 1
    block = (NV, NX, NY, NZ)
    vmem = lambda *shape: pltpu.VMEM(shape, jnp.float32)
    dma = lambda *shape: pltpu.SemaphoreType.DMA(shape)
    array = lambda *shape: jax.ShapeDtypeStruct(shape, jnp.float32)
    in_vmem = pl.BlockSpec(memory_space=pltpu.VMEM)
    in_hbm = pl.BlockSpec(memory_space=pltpu.HBM)
    parts = pl.pallas_call(
        functools.partial(kernel, sizes),
        out_shape=(
            array(*block),
            array(*block),
            array(2, NV, NY, NZ),
            array(2, CH, NV, ROWS, NZ),
            array(ROWS, NZ),
        ),
        in_specs=[in_hbm] * 4,
        out_specs=[in_vmem] * 5,
        scratch_shapes=[
            vmem(*block),
            vmem(*block),
            vmem(*block),
            vmem(*block),
            vmem(2, 2 * LANES, 2 * LANES),
            vmem(NX * NY, NX * NY),
            vmem(ROWS, NZ),
            vmem(2, 1, LANES),
            vmem(n_far, 1, LANES),
            vmem(n_near, 1, LANES),
            vmem(2, 2, NV, ROWS, NZ),
            vmem(2, 2, NY, LANES),
            vmem(2, 2, NV, ROWS, NZ),
            vmem(2, 2, NY, LANES),
            vmem(2, CH, NV, ROWS, NZ),
            vmem(2, NV, ROWS, NZ),
            vmem(2, NV, NY, LANES),
            dma(NX + 3),
            dma(2, 2, CH),
            dma(2, 2, CH),
            dma(2, 2, 2),
            dma(2, 2, 2),
            dma(n_far + n_near),
            dma(n_far + n_near),
        ],
        compiler_params=pltpu.CompilerParams(
            collective_id=0, has_side_effects=True, vmem_limit_bytes=32 * 2**20
        ),
        name="sections",
    )(*[pltpu.with_memory_space_constraint(x, pltpu.HBM) for x in (state, register, mat_z, mat_y)])
    return pl.pallas_call(
        finish,
        out_shape=(array(*block), array(*block)),
        in_specs=[in_vmem] * 5,
        out_specs=[in_hbm] * 2,
        scratch_shapes=[vmem(2, 2, NV, NY, NZ), dma(2, 3)],
        compiler_params=pltpu.CompilerParams(vmem_limit_bytes=16 * 2**20),
        name="finish",
    )(*parts)


def solution(mesh):
    gx, gy, gz = (mesh.shape[a] for a in ("gx", "gy", "gz"))
    sizes = (gx // 2, 2, gy, gz // 2, 2)
    torus = Mesh(mesh.devices.reshape(sizes), AXES)
    placed = P(None, ("gx_0", "gx_1"), "gy", ("gz_0", "gz_1"))
    return jax.shard_map(
        functools.partial(shards, sizes),
        mesh=torus,
        in_specs=(placed, placed),
        out_specs=(placed, placed),
        check_vma=False,
    )
```

```python
import functools
import math

import jax
import jax.numpy as jnp
import numpy as np
from jax import lax
from jax.experimental import pallas as pl
from jax.experimental.pallas import tpu as pltpu
from jax.sharding import Mesh
from jax.sharding import PartitionSpec as P

AXES = ("gx_0", "gx_1", "gy", "gz_0", "gz_1")
MESH = pl.DeviceIdType.MESH

GAMMA = 1.4
GM1 = 0.4
ELEM_WIDTH = 0.05
COURANT = 0.5
COEFFS = (
    (-567301805773.0 / 1357537059087.0, 5161836677717.0 / 13612068292357.0),
    (-2404267990393.0 / 2016746695238.0, 1720146321549.0 / 2090206949498.0),
)
NV = 5
N = 6
NX, NY, NZ = 6, 24, 384
ROWS = 8
CH = NY // ROWS
LANES = 128
SCALE = 2.0 / ELEM_WIDTH
FACE = SCALE * 15.0 * 0.5


def gll_derivative():
    seven = math.sqrt(7.0)
    inner = math.sqrt(1.0 / 3.0 - 2.0 * seven / 21.0)
    outer = math.sqrt(1.0 / 3.0 + 2.0 * seven / 21.0)
    points = np.array([-1.0, -outer, -inner, inner, outer, 1.0])
    count = len(points)
    weights = np.array(
        [np.prod([points[i] - points[j] for j in range(count) if j != i]) for i in range(count)]
    )
    table = np.zeros((count, count))
    for i in range(count):
        for j in range(count):
            if i != j:
                table[i, j] = weights[i] / weights[j] / (points[i] - points[j])
        table[i, i] = -np.sum(table[i])
    return table


DIFF = gll_derivative()


def line_operator(length):
    elems = length // N
    op = np.kron(np.eye(elems), -SCALE * DIFF)
    for e in range(elems - 1):
        last, first = N * e + N - 1, N * e + N
        for row in (last, first):
            op[row, last] += FACE
            op[row, first] -= FACE
    return op


def operators():
    along_z = line_operator(NZ).T
    cut = 2 * LANES - (2 * LANES) % N
    low = along_z[: 2 * LANES, : 2 * LANES].copy()
    low[:, cut:] = 0.0
    high = along_z[LANES:, LANES:].copy()
    high[:, : cut - LANES] = 0.0
    along_y = np.kron(np.eye(NX), line_operator(NY))
    return (
        jnp.asarray(np.stack([low, high]), jnp.float32),
        jnp.asarray(along_y, jnp.float32),
    )


def z_steps(nz):
    assert nz <= 8
    return (
        sorted({i % nz for i in (1, -1, 2, -2)} - {0}),
        sorted({i % nz for i in (0, 2, -2)}),
    )


def primitives(u):
    inv = 1.0 / u[0]
    vel = [u[1] * inv, u[2] * inv, u[3] * inv]
    press = GM1 * (u[4] - 0.5 * (u[1] * vel[0] + u[2] * vel[1] + u[3] * vel[2]))
    sound = jnp.sqrt(GAMMA * press * inv)
    return vel, press, sound


def flux(u, vel, press, d):
    parts = [u[1 + d], u[1] * vel[d], u[2] * vel[d], u[3] * vel[d], (u[4] + press) * vel[d]]
    parts[1 + d] = parts[1 + d] + press
    return parts


def face_terms(left, right, d):
    vel_l, press_l, sound_l = primitives(left)
    vel_r, press_r, sound_r = primitives(right)
    flux_l = flux(left, vel_l, press_l, d)
    flux_r = flux(right, vel_r, press_r, d)
    lam = FACE * jnp.maximum(jnp.abs(vel_l[d]) + sound_l, jnp.abs(vel_r[d]) + sound_r)
    a = [FACE * (fl - fr) for fl, fr in zip(flux_l, flux_r)]
    b = [lam * (r - l) for l, r in zip(left, right)]
    return a, b


def x_face(side, own, far):
    a, b = face_terms(far, own, 0) if side == 0 else face_terms(own, far, 0)
    return [p - q if side == 0 else p + q for p, q in zip(a, b)]


def advance(sec, k, u, dt, r):
    a, b = COEFFS[sec]
    new_k = a * k + dt * r
    return new_k, u + b * new_k


def kernel(
    sizes,
    state,
    register,
    mat_z,
    mat_y,
    u,
    k,
    edge,
    far_x,
    step,
    res,
    fx,
    fy,
    fz,
    mz,
    my,
    mask_z,
    top,
    top_1,
    top_2,
    top_3,
    y_pack,
    z_pack,
    y_halo,
    z_halo,
    near_x,
    y_corr,
    z_corr,
    load_sem,
    send_x,
    recv_x,
    send_yz,
    recv_yz,
    send_top,
    recv_top,
):
    nz, nxl, ny, nxh, nco = sizes
    z, xl, y, xh, co = (lax.axis_index(a) for a in AXES)

    def device(z_=z, xl_=xl, y_=y, xh_=xh, co_=co):
        return dict(zip(AXES, (z_, xl_, y_, xh_, co_)))

    def wrap(i, n):
        return lax.rem(i + n, n)

    other_xl, other_co = wrap(xl + 1, nxl), wrap(co + 1, nco)
    gx = (
        device(z_=wrap(z + xl - 1, nz), xl_=other_xl),
        device(z_=wrap(z + xl, nz), xl_=other_xl),
    )
    gy = (device(y_=wrap(y - 1, ny)), device(y_=wrap(y + 1, ny)))
    gz = (
        device(xh_=wrap(xh + co - 1, nxh), co_=other_co),
        device(xh_=wrap(xh + co, nxh), co_=other_co),
    )
    def at(i, a, b, c):
        return device(
            z_=wrap(z + i, nz), xh_=wrap(xh + a, nxh), xl_=wrap(xl + b, nxl), co_=wrap(co + c, nco)
        )

    steps_1, steps_2 = z_steps(nz)
    group_1 = [device(z_=wrap(z + i, nz)) for i in steps_1]
    group_2 = [
        at(i, a, b, c)
        for i in steps_2
        for a in range(nxh)
        for b in range(nxl)
        for c in range(nco)
        if i or a or b or c
    ]
    group_3 = [device(y_=wrap(y + i, ny)) for i in range(1, ny)]
    group_x = [
        at(0, a, b, c) for a in range(nxh) for b in range(nxl) for c in range(nco) if a or b or c
    ]
    diagonal = device(z_=wrap(z + 2 * xl - 1, nz), xl_=other_xl)

    loads = [
        pltpu.make_async_copy(mat_z, mz, load_sem.at[NX]),
        pltpu.make_async_copy(mat_y, my, load_sem.at[NX + 1]),
        pltpu.make_async_copy(register, k, load_sem.at[NX + 2]),
    ]

    def load_plane(x):
        return pltpu.make_async_copy(state.at[:, x], u.at[:, x], load_sem.at[x])

    for x in range(NX):
        load_plane(x).start()
    for load in loads:
        load.start()
    barrier = pltpu.get_barrier_semaphore()
    partners = group_1 + group_x + group_3 + [diagonal]
    for partner in partners:
        pl.semaphore_signal(barrier, inc=1, device_id=partner, device_id_type=MESH)

    lane = lax.broadcasted_iota(jnp.int32, (ROWS, NZ), 1)
    lane_f = lane.astype(jnp.float32)
    place = lane_f - N * jnp.floor((lane_f + 0.5) * (1.0 / N))
    mask_z[...] = jnp.where((place > N - 1.5) & (lane < NZ - 1), FACE, 0.0)
    row = lax.broadcasted_iota(jnp.int32, (ROWS, NZ), 0)
    lane_1 = lax.broadcasted_iota(jnp.int32, (NY, LANES), 1)

    def chunk(ref, x, c):
        return [ref[v, x, pl.ds(ROWS * c, ROWS), :] for v in range(NV)]

    def speed_body(x, carry):
        load_plane(x).wait()
        for c in range(CH):
            w = chunk(u, x, c)
            vel, press, sound = primitives(w)
            mom = jnp.sqrt(w[1] * w[1] + w[2] * w[2] + w[3] * w[3])
            s = mom * (1.0 / w[0]) + sound
            carry = jnp.maximum(carry, s)
        return carry

    best = lax.fori_loop(0, NX, speed_body, jnp.zeros((ROWS, NZ), jnp.float32))
    best = jnp.maximum(
        jnp.maximum(best[:, :LANES], best[:, LANES : 2 * LANES]), best[:, 2 * LANES :]
    )
    top[0] = jnp.max(best, axis=0, keepdims=True)

    def pack(sec):
        def body(v, carry):
            low, high = carry
            for x in range(NX):
                y_pack[sec, 0, v, x : x + 1, :] = u[v, x, 0:1, :]
                y_pack[sec, 1, v, x : x + 1, :] = u[v, x, NY - 1 : NY, :]
                here = lane_1 == v * NX + x
                low = jnp.where(here, u[v, x, :, 0:LANES][:, 0:1], low)
                high = jnp.where(here, u[v, x, :, NZ - LANES : NZ][:, LANES - 1 : LANES], high)
            for x in range(NX, ROWS):
                y_pack[sec, 0, v, x : x + 1, :] = u[v, 0, 0:1, :]
                y_pack[sec, 1, v, x : x + 1, :] = u[v, 0, NY - 1 : NY, :]
            return low, high

        ones = jnp.ones((NY, LANES), jnp.float32)
        low, high = lax.fori_loop(0, NV, body, (ones, ones))
        z_pack[sec, 0] = low
        z_pack[sec, 1] = high

    def remote(src, dst, send, recv, to):
        return pltpu.make_async_remote_copy(
            src_ref=src,
            dst_ref=dst,
            send_sem=send,
            recv_sem=recv,
            device_id=to,
            device_id_type=MESH,
        )

    def x_copy(sec, side, c):
        src = state if sec == 0 else u
        return remote(
            src.at[:, 0 if side == 0 else NX - 1, pl.ds(ROWS * c, ROWS), :],
            (far_x if sec else near_x).at[1 - side, c],
            send_x.at[sec, side, c],
            recv_x.at[sec, 1 - side, c],
            gx[side],
        )

    def y_copy(sec, side):
        return remote(
            y_pack.at[sec, side],
            y_halo.at[sec, 1 - side],
            send_yz.at[sec, 0, side],
            recv_yz.at[sec, 0, 1 - side],
            gy[side],
        )

    def z_copy(sec, side):
        return remote(
            z_pack.at[sec, side],
            z_halo.at[sec, 1 - side],
            send_yz.at[sec, 1, side],
            recv_yz.at[sec, 1, 1 - side],
            gz[side],
        )

    def top_copies(stage, group, slots, first):
        return [
            remote(top.at[stage], slots.at[i], send_top.at[first + i], recv_top.at[first + i], to)
            for i, to in enumerate(group)
        ]

    tops_1 = top_copies(0, group_1, top_1, 0)
    tops_2 = top_copies(1, group_2, top_2, len(group_1))
    tops_3 = top_copies(2, group_3, top_3, len(group_1) + len(group_2))

    def start(copies):
        for copy in copies:
            copy.start()

    def gather_top(stage, copies, slots):
        value = top[stage]
        for i, copy in enumerate(copies):
            copy.wait_recv()
            value = jnp.maximum(value, slots[i])
        return value

    def y_z_copies(sec):
        return [z_copy(sec, 0), z_copy(sec, 1), y_copy(sec, 0), y_copy(sec, 1)]

    def fluxes_and_jumps():
        def body(x, carry):
            for c in range(CH):
                w = chunk(u, x, c)
                vel, press, sound = primitives(w)
                rows = pl.ds(ROWS * c, ROWS)
                for d, to in enumerate((fx, fy, fz)):
                    for v, part in enumerate(flux(w, vel, press, d)):
                        to[v, x, rows, :] = part
                s_y = jnp.abs(vel[1]) + sound
                s_z = jnp.abs(vel[2]) + sound
                lam_y = jnp.where(
                    row == N - 1 - 2 * c,
                    FACE * jnp.maximum(s_y, pltpu.roll(s_y, ROWS - 1, 0)),
                    0.0,
                )
                lam_z = mask_z[...] * jnp.maximum(s_z, pltpu.roll(s_z, NZ - 1, 1))
                for v in range(NV):
                    t_y = lam_y * (pltpu.roll(w[v], ROWS - 1, 0) - w[v])
                    t_z = lam_z * (pltpu.roll(w[v], NZ - 1, 1) - w[v])
                    res[v, x, rows, :] = (t_y - pltpu.roll(t_y, 1, 0)) + (
                        t_z - pltpu.roll(t_z, 1, 1)
                    )
            return carry

        lax.fori_loop(0, NX, body, 0)

    def dot(a, b):
        return jnp.dot(
            a, b, precision=lax.Precision.HIGHEST, preferred_element_type=jnp.float32
        )

    def lines_y_z():
        def body(v, carry):
            along_z = fz[v].reshape(NX * NY, NZ)
            low = dot(along_z[:, : 2 * LANES], mz[0])
            high = dot(along_z[:, LANES:], mz[1])
            both = jnp.concatenate(
                [low[:, :LANES], low[:, LANES:] + high[:, :LANES], high[:, LANES:]], axis=1
            )
            along_y = dot(my[...], fy[v].reshape(NX * NY, NZ))
            res[v] = res[v] + (both + along_y).reshape(NX, NY, NZ)
            return carry

        lax.fori_loop(0, NV, body, 0)

    def lines_x():
        half = N // 2
        even = [[-SCALE * 0.5 * (DIFF[i, j] + DIFF[i, N - 1 - j]) for j in range(half)] for i in range(half)]
        odd = [[-SCALE * 0.5 * (DIFF[i, j] - DIFF[i, N - 1 - j]) for j in range(half)] for i in range(half)]

        def body(v, carry):
            for c in range(CH):
                rows = pl.ds(ROWS * c, ROWS)
                f = [fx[v, x, rows, :] for x in range(NX)]
                plus = [f[j] + f[N - 1 - j] for j in range(half)]
                minus = [f[j] - f[N - 1 - j] for j in range(half)]
                for i in range(half):
                    a = sum(even[i][j] * plus[j] for j in range(half))
                    b = sum(odd[i][j] * minus[j] for j in range(half))
                    res[v, i, rows, :] += b + a
                    res[v, N - 1 - i, rows, :] += b - a
            return carry

        lax.fori_loop(0, NV, body, 0)

    def y_z_faces(sec):
        for side in (0, 1):
            y_copy(sec, 1 - side).wait_recv()
            own = [y_pack[sec, side, v] for v in range(NV)]
            far = [y_halo[sec, side, v] for v in range(NV)]
            a, b = face_terms(far, own, 1) if side == 0 else face_terms(own, far, 1)
            for v in range(NV):
                y_corr[side, v] = a[v] - b[v] if side == 0 else a[v] + b[v]
            z_copy(sec, 1 - side).wait_recv()

            def part(ref, v):
                tile = ref[sec, side]
                return tile if v == 0 else pltpu.roll(tile, LANES - NX * v, 1)

            own = [part(z_pack, v) for v in range(NV)]
            far = [part(z_halo, v) for v in range(NV)]
            a, b = face_terms(far, own, 2) if side == 0 else face_terms(own, far, 2)
            for v in range(NV):
                z_corr[side, v] = a[v] - b[v] if side == 0 else a[v] + b[v]

        def body(v, carry):
            for x in range(NX):
                res[v, x, 0:1, :] += y_corr[0, v, x : x + 1, :]
                res[v, x, NY - 1 : NY, :] += y_corr[1, v, x : x + 1, :]
                low = z_corr[0, v][:, x : x + 1]
                high = z_corr[1, v][:, x : x + 1]
                res[v, x, :, 0:LANES] += jnp.where(lane_1 == 0, low, 0.0)
                res[v, x, :, NZ - LANES : NZ] += jnp.where(lane_1 == LANES - 1, high, 0.0)
            return carry

        lax.fori_loop(0, NV, body, 0)

    def update(sec, x, c, extra):
        rows = pl.ds(ROWS * c, ROWS)
        for v in range(NV):
            r = res[v, x, rows, :]
            if extra is not None:
                r = r + extra[v]
            new_k, new_u = advance(sec, k[v, x, rows, :], u[v, x, rows, :], step[...], r)
            k[v, x, rows, :] = new_k
            u[v, x, rows, :] = new_u

    def update_boundary(side, c):
        x_copy(0, 1 - side, c).wait_recv()
        x = 0 if side == 0 else NX - 1
        own = chunk(u, x, c)
        far = [near_x[side, c, v] for v in range(NV)]
        update(0, x, c, x_face(side, own, far))

    def update_interior(sec):
        def body(x, carry):
            for c in range(CH):
                update(sec, x, c, None)
            return carry

        lax.fori_loop(1, NX - 1, body, 0)

    pl.semaphore_wait(barrier, len(partners))
    start(tops_1)
    start([x_copy(0, 0, 0), x_copy(0, 1, 0)])
    pack(0)
    start(y_z_copies(0))
    fluxes_and_jumps()
    top[1] = gather_top(0, tops_1, top_1)
    start(tops_2)
    for c in range(1, CH):
        start([x_copy(0, 0, c), x_copy(0, 1, c)])
    loads[0].wait()
    loads[1].wait()
    lines_y_z()
    top[2] = gather_top(1, tops_2, top_2)
    start(tops_3)
    lines_x()
    y_z_faces(0)
    value = gather_top(2, tops_3, top_3)
    value = jnp.max(jnp.broadcast_to(value, (ROWS, LANES)), axis=1, keepdims=True)
    step[...] = jnp.broadcast_to(COURANT * ELEM_WIDTH / (11.0 * value), (ROWS, NZ))
    loads[2].wait()

    for c in range(CH):
        for side in (0, 1):
            update_boundary(side, c)
            if c < CH - 1:
                x_copy(1, side, c).start()
    update_interior(0)
    pack(1)
    start(y_z_copies(1))
    start([x_copy(1, 0, CH - 1), x_copy(1, 1, CH - 1)])

    fluxes_and_jumps()
    lines_y_z()
    lines_x()
    y_z_faces(1)
    update_interior(1)
    for v in range(NV):
        edge[0, v] = res[v, 0]
        edge[1, v] = res[v, NX - 1]
    for c in range(CH):
        for side in (0, 1):
            x_copy(1, side, c).wait_recv()

    for copy in tops_1 + tops_2 + tops_3:
        copy.wait_send()
    for sec in (0, 1):
        for copy in y_z_copies(sec):
            copy.wait_send()
        for c in range(CH):
            for side in (0, 1):
                x_copy(sec, side, c).wait_send()


def finish(u, k, edge, far_x, step, out_state, out_register, done, sem):
    inner = [
        pltpu.make_async_copy(
            src.at[:, pl.ds(1, NX - 2)], dst.at[:, pl.ds(1, NX - 2)], sem.at[i, 0]
        )
        for i, (src, dst) in enumerate(((u, out_state), (k, out_register)))
    ]
    for copy in inner:
        copy.start()
    outer = []
    for side in (0, 1):
        x = 0 if side == 0 else NX - 1
        for c in range(CH):
            rows = pl.ds(ROWS * c, ROWS)
            own = [u[v, x, rows, :] for v in range(NV)]
            far = [far_x[side, c, v] for v in range(NV)]
            extra = x_face(side, own, far)
            for v in range(NV):
                new_k, new_u = advance(
                    1, k[v, x, rows, :], own[v], step[...], edge[side, v, rows, :] + extra[v]
                )
                done[0, side, v, rows, :] = new_u
                done[1, side, v, rows, :] = new_k
        for i, dst in enumerate((out_state, out_register)):
            copy = pltpu.make_async_copy(done.at[i, side], dst.at[:, x], sem.at[i, 1 + side])
            copy.start()
            outer.append(copy)
    for copy in inner + outer:
        copy.wait()


def shards(sizes, state, register):
    mat_z, mat_y = operators()
    nz, nxl, ny, nxh, nco = sizes
    steps_1, steps_2 = z_steps(nz)
    counts = (len(steps_1), len(steps_2) * nxh * nxl * nco - 1, ny - 1)
    block = (NV, NX, NY, NZ)
    vmem = lambda *shape: pltpu.VMEM(shape, jnp.float32)
    dma = lambda *shape: pltpu.SemaphoreType.DMA(shape)
    array = lambda *shape: jax.ShapeDtypeStruct(shape, jnp.float32)
    in_vmem = pl.BlockSpec(memory_space=pltpu.VMEM)
    in_hbm = pl.BlockSpec(memory_space=pltpu.HBM)
    parts = pl.pallas_call(
        functools.partial(kernel, sizes),
        out_shape=(
            array(*block),
            array(*block),
            array(2, NV, NY, NZ),
            array(2, CH, NV, ROWS, NZ),
            array(ROWS, NZ),
        ),
        in_specs=[in_hbm] * 4,
        out_specs=[in_vmem] * 5,
        scratch_shapes=[
            vmem(*block),
            vmem(*block),
            vmem(*block),
            vmem(*block),
            vmem(2, 2 * LANES, 2 * LANES),
            vmem(NX * NY, NX * NY),
            vmem(ROWS, NZ),
            vmem(3, 1, LANES),
            vmem(counts[0], 1, LANES),
            vmem(counts[1], 1, LANES),
            vmem(counts[2], 1, LANES),
            vmem(2, 2, NV, ROWS, NZ),
            vmem(2, 2, NY, LANES),
            vmem(2, 2, NV, ROWS, NZ),
            vmem(2, 2, NY, LANES),
            vmem(2, CH, NV, ROWS, NZ),
            vmem(2, NV, ROWS, NZ),
            vmem(2, NV, NY, LANES),
            dma(NX + 3),
            dma(2, 2, CH),
            dma(2, 2, CH),
            dma(2, 2, 2),
            dma(2, 2, 2),
            dma(sum(counts)),
            dma(sum(counts)),
        ],
        compiler_params=pltpu.CompilerParams(
            collective_id=0, has_side_effects=True, vmem_limit_bytes=32 * 2**20
        ),
        name="sections",
    )(*[pltpu.with_memory_space_constraint(x, pltpu.HBM) for x in (state, register, mat_z, mat_y)])
    return pl.pallas_call(
        finish,
        out_shape=(array(*block), array(*block)),
        in_specs=[in_vmem] * 5,
        out_specs=[in_hbm] * 2,
        scratch_shapes=[vmem(2, 2, NV, NY, NZ), dma(2, 3)],
        compiler_params=pltpu.CompilerParams(vmem_limit_bytes=16 * 2**20),
        name="finish",
    )(*parts)


def solution(mesh):
    gx, gy, gz = (mesh.shape[a] for a in ("gx", "gy", "gz"))
    sizes = (gx // 2, 2, gy, gz // 2, 2)
    torus = Mesh(mesh.devices.reshape(sizes), AXES)
    placed = P(None, ("gx_0", "gx_1"), "gy", ("gz_0", "gz_1"))
    return jax.shard_map(
        functools.partial(shards, sizes),
        mesh=torus,
        in_specs=(placed, placed),
        out_specs=(placed, placed),
        check_vma=False,
    )
```

```python
import functools
import math

import jax
import jax.numpy as jnp
import numpy as np
from jax import lax
from jax.experimental import pallas as pl
from jax.experimental.pallas import tpu as pltpu
from jax.sharding import Mesh
from jax.sharding import PartitionSpec as P

AXES = ("gx_0", "gx_1", "gy", "gz_0", "gz_1")
MESH = pl.DeviceIdType.MESH

GAMMA = 1.4
GM1 = 0.4
ELEM_WIDTH = 0.05
COURANT = 0.5
COEFFS = (
    (-567301805773.0 / 1357537059087.0, 5161836677717.0 / 13612068292357.0),
    (-2404267990393.0 / 2016746695238.0, 1720146321549.0 / 2090206949498.0),
)
NV = 5
N = 6
NX, NY, NZ = 6, 24, 384
ROWS = 8
CH = NY // ROWS
LANES = 128
SCALE = 2.0 / ELEM_WIDTH
FACE = SCALE * 15.0 * 0.5


def gll_derivative():
    seven = math.sqrt(7.0)
    inner = math.sqrt(1.0 / 3.0 - 2.0 * seven / 21.0)
    outer = math.sqrt(1.0 / 3.0 + 2.0 * seven / 21.0)
    points = np.array([-1.0, -outer, -inner, inner, outer, 1.0])
    count = len(points)
    weights = np.array(
        [np.prod([points[i] - points[j] for j in range(count) if j != i]) for i in range(count)]
    )
    table = np.zeros((count, count))
    for i in range(count):
        for j in range(count):
            if i != j:
                table[i, j] = weights[i] / weights[j] / (points[i] - points[j])
        table[i, i] = -np.sum(table[i])
    return table


DIFF = gll_derivative()


def line_operator(length):
    elems = length // N
    op = np.kron(np.eye(elems), -SCALE * DIFF)
    for e in range(elems - 1):
        last, first = N * e + N - 1, N * e + N
        for row in (last, first):
            op[row, last] += FACE
            op[row, first] -= FACE
    return op


def halves(x):
    top = x.astype(jnp.bfloat16)
    return top, (x - top.astype(jnp.float32)).astype(jnp.bfloat16)


def operators():
    along_z = line_operator(NZ).T
    cut = 2 * LANES - (2 * LANES) % N
    low = along_z[: 2 * LANES, : 2 * LANES].copy()
    low[:, cut:] = 0.0
    high = along_z[LANES:, LANES:].copy()
    high[:, : cut - LANES] = 0.0
    along_y = np.kron(np.eye(NX), line_operator(NY))
    return tuple(jnp.stack(halves(jnp.asarray(m, jnp.float32))) for m in (np.stack([low, high]), along_y))


def z_steps(nz):
    assert nz <= 8
    return (
        sorted({i % nz for i in (1, -1, 2, -2)} - {0}),
        sorted({i % nz for i in (0, 2, -2)}),
    )


def primitives(u):
    inv = 1.0 / u[0]
    vel = [u[1] * inv, u[2] * inv, u[3] * inv]
    press = GM1 * (u[4] - 0.5 * (u[1] * vel[0] + u[2] * vel[1] + u[3] * vel[2]))
    sound = jnp.sqrt(GAMMA * press * inv)
    return vel, press, sound


def flux(u, vel, press, d):
    parts = [u[1 + d], u[1] * vel[d], u[2] * vel[d], u[3] * vel[d], (u[4] + press) * vel[d]]
    parts[1 + d] = parts[1 + d] + press
    return parts


def face_terms(left, right, d):
    vel_l, press_l, sound_l = primitives(left)
    vel_r, press_r, sound_r = primitives(right)
    flux_l = flux(left, vel_l, press_l, d)
    flux_r = flux(right, vel_r, press_r, d)
    lam = FACE * jnp.maximum(jnp.abs(vel_l[d]) + sound_l, jnp.abs(vel_r[d]) + sound_r)
    a = [FACE * (fl - fr) for fl, fr in zip(flux_l, flux_r)]
    b = [lam * (r - l) for l, r in zip(left, right)]
    return a, b


def x_face(side, own, far):
    a, b = face_terms(far, own, 0) if side == 0 else face_terms(own, far, 0)
    return [p - q if side == 0 else p + q for p, q in zip(a, b)]


def advance(sec, k, u, dt, r):
    a, b = COEFFS[sec]
    new_k = a * k + dt * r
    return new_k, u + b * new_k


def kernel(
    sizes,
    state,
    register,
    mat_z,
    mat_y,
    u,
    k,
    edge,
    far_x,
    far_ab,
    step,
    res,
    fx,
    fy,
    fz,
    mz,
    my,
    mask_z,
    top,
    top_1,
    top_2,
    top_3,
    y_pack,
    z_pack,
    y_halo,
    z_halo,
    near_x,
    ab,
    y_corr,
    z_corr,
    load_sem,
    send_x,
    recv_x,
    send_ab,
    recv_ab,
    send_yz,
    recv_yz,
    send_top,
    recv_top,
):
    nz, nxl, ny, nxh, nco = sizes
    z, xl, y, xh, co = (lax.axis_index(a) for a in AXES)

    def device(z_=z, xl_=xl, y_=y, xh_=xh, co_=co):
        return dict(zip(AXES, (z_, xl_, y_, xh_, co_)))

    def wrap(i, n):
        return lax.rem(i + n, n)

    other_xl, other_co = wrap(xl + 1, nxl), wrap(co + 1, nco)
    gx = (
        device(z_=wrap(z + xl - 1, nz), xl_=other_xl),
        device(z_=wrap(z + xl, nz), xl_=other_xl),
    )
    gy = (device(y_=wrap(y - 1, ny)), device(y_=wrap(y + 1, ny)))
    gz = (
        device(xh_=wrap(xh + co - 1, nxh), co_=other_co),
        device(xh_=wrap(xh + co, nxh), co_=other_co),
    )
    def at(i, a, b, c):
        return device(
            z_=wrap(z + i, nz), xh_=wrap(xh + a, nxh), xl_=wrap(xl + b, nxl), co_=wrap(co + c, nco)
        )

    steps_1, steps_2 = z_steps(nz)
    group_1 = [device(z_=wrap(z + i, nz)) for i in steps_1]
    group_2 = [
        at(i, a, b, c)
        for i in steps_2
        for a in range(nxh)
        for b in range(nxl)
        for c in range(nco)
        if i or a or b or c
    ]
    group_3 = [device(y_=wrap(y + i, ny)) for i in range(1, ny)]
    group_x = [
        at(0, a, b, c) for a in range(nxh) for b in range(nxl) for c in range(nco) if a or b or c
    ]
    diagonal = device(z_=wrap(z + 2 * xl - 1, nz), xl_=other_xl)

    loads = [
        pltpu.make_async_copy(mat_z, mz, load_sem.at[NX]),
        pltpu.make_async_copy(mat_y, my, load_sem.at[NX + 1]),
        pltpu.make_async_copy(register, k, load_sem.at[NX + 2]),
    ]

    def load_plane(x):
        return pltpu.make_async_copy(state.at[:, x], u.at[:, x], load_sem.at[x])

    for x in range(NX):
        load_plane(x).start()
    for load in loads:
        load.start()
    barrier = pltpu.get_barrier_semaphore()
    partners = group_1 + group_x + group_3 + [diagonal]
    for partner in partners:
        pl.semaphore_signal(barrier, inc=1, device_id=partner, device_id_type=MESH)

    lane = lax.broadcasted_iota(jnp.int32, (ROWS, NZ), 1)
    lane_f = lane.astype(jnp.float32)
    place = lane_f - N * jnp.floor((lane_f + 0.5) * (1.0 / N))
    mask_z[...] = jnp.where((place > N - 1.5) & (lane < NZ - 1), FACE, 0.0)
    row = lax.broadcasted_iota(jnp.int32, (ROWS, NZ), 0)
    lane_1 = lax.broadcasted_iota(jnp.int32, (NY, LANES), 1)

    def chunk(ref, x, c):
        return [ref[v, x, pl.ds(ROWS * c, ROWS), :] for v in range(NV)]

    def speed_body(x, carry):
        load_plane(x).wait()
        for c in range(CH):
            w = chunk(u, x, c)
            vel, press, sound = primitives(w)
            mom = jnp.sqrt(w[1] * w[1] + w[2] * w[2] + w[3] * w[3])
            s = mom * (1.0 / w[0]) + sound
            carry = jnp.maximum(carry, s)
        return carry

    best = lax.fori_loop(0, NX, speed_body, jnp.zeros((ROWS, NZ), jnp.float32))
    best = jnp.maximum(
        jnp.maximum(best[:, :LANES], best[:, LANES : 2 * LANES]), best[:, 2 * LANES :]
    )
    top[0] = jnp.max(best, axis=0, keepdims=True)

    def pack(sec):
        def body(v, carry):
            low, high = carry
            for x in range(NX):
                y_pack[sec, 0, v, x : x + 1, :] = u[v, x, 0:1, :]
                y_pack[sec, 1, v, x : x + 1, :] = u[v, x, NY - 1 : NY, :]
                here = lane_1 == v * NX + x
                low = jnp.where(here, u[v, x, :, 0:LANES][:, 0:1], low)
                high = jnp.where(here, u[v, x, :, NZ - LANES : NZ][:, LANES - 1 : LANES], high)
            for x in range(NX, ROWS):
                y_pack[sec, 0, v, x : x + 1, :] = u[v, 0, 0:1, :]
                y_pack[sec, 1, v, x : x + 1, :] = u[v, 0, NY - 1 : NY, :]
            return low, high

        ones = jnp.ones((NY, LANES), jnp.float32)
        low, high = lax.fori_loop(0, NV, body, (ones, ones))
        z_pack[sec, 0] = low
        z_pack[sec, 1] = high

    def remote(src, dst, send, recv, to):
        return pltpu.make_async_remote_copy(
            src_ref=src,
            dst_ref=dst,
            send_sem=send,
            recv_sem=recv,
            device_id=to,
            device_id_type=MESH,
        )

    def x_copy(sec, side, c):
        src = state if sec == 0 else u
        return remote(
            src.at[:, 0 if side == 0 else NX - 1, pl.ds(ROWS * c, ROWS), :],
            far_x.at[1 - side, c - 1] if sec else near_x.at[1 - side, c],
            send_x.at[sec, side, c],
            recv_x.at[sec, 1 - side, c],
            gx[side],
        )

    def ab_copy(part, side):
        return remote(
            ab.at[part, side],
            far_ab.at[part, 1 - side],
            send_ab.at[part, side],
            recv_ab.at[part, 1 - side],
            gx[side],
        )

    def y_copy(sec, side):
        return remote(
            y_pack.at[sec, side],
            y_halo.at[sec, 1 - side],
            send_yz.at[sec, 0, side],
            recv_yz.at[sec, 0, 1 - side],
            gy[side],
        )

    def z_copy(sec, side):
        return remote(
            z_pack.at[sec, side],
            z_halo.at[sec, 1 - side],
            send_yz.at[sec, 1, side],
            recv_yz.at[sec, 1, 1 - side],
            gz[side],
        )

    def top_copies(stage, group, slots, first):
        return [
            remote(top.at[stage], slots.at[i], send_top.at[first + i], recv_top.at[first + i], to)
            for i, to in enumerate(group)
        ]

    tops_1 = top_copies(0, group_1, top_1, 0)
    tops_2 = top_copies(1, group_2, top_2, len(group_1))
    tops_3 = top_copies(2, group_3, top_3, len(group_1) + len(group_2))

    def start(copies):
        for copy in copies:
            copy.start()

    def gather_top(stage, copies, slots):
        value = top[stage]
        for i, copy in enumerate(copies):
            copy.wait_recv()
            value = jnp.maximum(value, slots[i])
        return value

    def y_z_copies(sec):
        return [z_copy(sec, 0), z_copy(sec, 1), y_copy(sec, 0), y_copy(sec, 1)]

    def fluxes_and_jumps():
        def body(x, carry):
            for c in range(CH):
                w = chunk(u, x, c)
                vel, press, sound = primitives(w)
                rows = pl.ds(ROWS * c, ROWS)
                for d, to in enumerate((fx, fy, fz)):
                    for v, part in enumerate(flux(w, vel, press, d)):
                        to[v, x, rows, :] = part
                s_y = jnp.abs(vel[1]) + sound
                s_z = jnp.abs(vel[2]) + sound
                lam_y = jnp.where(
                    row == N - 1 - 2 * c,
                    FACE * jnp.maximum(s_y, pltpu.roll(s_y, ROWS - 1, 0)),
                    0.0,
                )
                lam_z = mask_z[...] * jnp.maximum(s_z, pltpu.roll(s_z, NZ - 1, 1))
                for v in range(NV):
                    t_y = lam_y * (pltpu.roll(w[v], ROWS - 1, 0) - w[v])
                    t_z = lam_z * (pltpu.roll(w[v], NZ - 1, 1) - w[v])
                    res[v, x, rows, :] = (t_y - pltpu.roll(t_y, 1, 0)) + (
                        t_z - pltpu.roll(t_z, 1, 1)
                    )
            return carry

        lax.fori_loop(0, NX, body, 0)

    def dot(a, b):
        (a_top, a_rest), (b_top, b_rest) = a, b
        one = lambda p, q: jnp.dot(p, q, preferred_element_type=jnp.float32)
        return one(a_top, b_top) + (one(a_top, b_rest) + one(a_rest, b_top))

    def lines_y_z():
        def body(v, carry):
            along_z = halves(fz[v].reshape(NX * NY, NZ))
            low = dot([p[:, : 2 * LANES] for p in along_z], (mz[0, 0], mz[1, 0]))
            high = dot([p[:, LANES:] for p in along_z], (mz[0, 1], mz[1, 1]))
            both = jnp.concatenate(
                [low[:, :LANES], low[:, LANES:] + high[:, :LANES], high[:, LANES:]], axis=1
            )
            along_y = dot((my[0], my[1]), halves(fy[v].reshape(NX * NY, NZ)))
            res[v] = res[v] + (both + along_y).reshape(NX, NY, NZ)
            return carry

        lax.fori_loop(0, NV, body, 0)

    def lines_x():
        half = N // 2
        even = [[-SCALE * 0.5 * (DIFF[i, j] + DIFF[i, N - 1 - j]) for j in range(half)] for i in range(half)]
        odd = [[-SCALE * 0.5 * (DIFF[i, j] - DIFF[i, N - 1 - j]) for j in range(half)] for i in range(half)]

        def body(v, carry):
            for c in range(CH):
                rows = pl.ds(ROWS * c, ROWS)
                f = [fx[v, x, rows, :] for x in range(NX)]
                plus = [f[j] + f[N - 1 - j] for j in range(half)]
                minus = [f[j] - f[N - 1 - j] for j in range(half)]
                for i in range(half):
                    a = sum(even[i][j] * plus[j] for j in range(half))
                    b = sum(odd[i][j] * minus[j] for j in range(half))
                    res[v, i, rows, :] += b + a
                    res[v, N - 1 - i, rows, :] += b - a
            return carry

        lax.fori_loop(0, NV, body, 0)

    def y_z_faces(sec):
        for side in (0, 1):
            y_copy(sec, 1 - side).wait_recv()
            own = [y_pack[sec, side, v] for v in range(NV)]
            far = [y_halo[sec, side, v] for v in range(NV)]
            a, b = face_terms(far, own, 1) if side == 0 else face_terms(own, far, 1)
            for v in range(NV):
                y_corr[side, v] = a[v] - b[v] if side == 0 else a[v] + b[v]
            z_copy(sec, 1 - side).wait_recv()

            def part(ref, v):
                tile = ref[sec, side]
                return tile if v == 0 else pltpu.roll(tile, LANES - NX * v, 1)

            own = [part(z_pack, v) for v in range(NV)]
            far = [part(z_halo, v) for v in range(NV)]
            a, b = face_terms(far, own, 2) if side == 0 else face_terms(own, far, 2)
            for v in range(NV):
                z_corr[side, v] = a[v] - b[v] if side == 0 else a[v] + b[v]

        def body(v, carry):
            for x in range(NX):
                res[v, x, 0:1, :] += y_corr[0, v, x : x + 1, :]
                res[v, x, NY - 1 : NY, :] += y_corr[1, v, x : x + 1, :]
                low = z_corr[0, v][:, x : x + 1]
                high = z_corr[1, v][:, x : x + 1]
                res[v, x, :, 0:LANES] += jnp.where(lane_1 == 0, low, 0.0)
                res[v, x, :, NZ - LANES : NZ] += jnp.where(lane_1 == LANES - 1, high, 0.0)
            return carry

        lax.fori_loop(0, NV, body, 0)

    def update(sec, x, c, extra):
        rows = pl.ds(ROWS * c, ROWS)
        for v in range(NV):
            r = res[v, x, rows, :]
            if extra is not None:
                r = r + extra[v]
            new_k, new_u = advance(sec, k[v, x, rows, :], u[v, x, rows, :], step[...], r)
            k[v, x, rows, :] = new_k
            u[v, x, rows, :] = new_u

    def plane(side):
        return 0 if side == 0 else NX - 1

    def known_part(side):
        a, b = COEFFS[0]
        rows = pl.ds(0, ROWS)
        for v in range(NV):
            ab[0, side, v] = u[v, plane(side), rows, :] + b * (a * k[v, plane(side), rows, :])
        ab_copy(0, side).start()

    def step_part(side):
        extra = boundary_terms(side, 0)
        for v in range(NV):
            r = res[v, plane(side), 0:ROWS, :] + extra[v]
            res[v, plane(side), 0:ROWS, :] = r
            ab[1, side, v] = COEFFS[0][1] * r
        ab_copy(1, side).start()

    def boundary_terms(side, c):
        x_copy(0, 1 - side, c).wait_recv()
        return x_face(side, chunk(u, plane(side), c), [near_x[side, c, v] for v in range(NV)])

    def update_interior(sec):
        def body(x, carry):
            for c in range(CH):
                update(sec, x, c, None)
            return carry

        lax.fori_loop(1, NX - 1, body, 0)

    pl.semaphore_wait(barrier, len(partners))
    start(tops_1)
    start([x_copy(0, 0, 0), x_copy(0, 1, 0)])
    pack(0)
    start(y_z_copies(0))
    fluxes_and_jumps()
    top[1] = gather_top(0, tops_1, top_1)
    start(tops_2)
    for c in range(1, CH):
        start([x_copy(0, 0, c), x_copy(0, 1, c)])
    loads[2].wait()
    for side in (0, 1):
        known_part(side)
    loads[0].wait()
    loads[1].wait()
    lines_y_z()
    top[2] = gather_top(1, tops_2, top_2)
    start(tops_3)
    lines_x()
    y_z_faces(0)
    for side in (0, 1):
        step_part(side)
    value = gather_top(2, tops_3, top_3)
    value = jnp.max(jnp.broadcast_to(value, (ROWS, LANES)), axis=1, keepdims=True)
    step[...] = jnp.broadcast_to(COURANT * ELEM_WIDTH / (11.0 * value), (ROWS, NZ))

    for c in (*range(1, CH), 0):
        for side in (0, 1):
            update(0, plane(side), c, boundary_terms(side, c) if c else None)
            if 0 < c < CH - 1:
                x_copy(1, side, c).start()
    update_interior(0)
    pack(1)
    start(y_z_copies(1))
    start([x_copy(1, 0, CH - 1), x_copy(1, 1, CH - 1)])

    fluxes_and_jumps()
    lines_y_z()
    lines_x()
    y_z_faces(1)
    update_interior(1)
    for v in range(NV):
        edge[0, v] = res[v, 0]
        edge[1, v] = res[v, NX - 1]
    for side in (0, 1):
        for part in (0, 1):
            ab_copy(part, side).wait_recv()
        for c in range(1, CH):
            x_copy(1, side, c).wait_recv()

    for copy in tops_1 + tops_2 + tops_3:
        copy.wait_send()
    for sec in (0, 1):
        for copy in y_z_copies(sec):
            copy.wait_send()
        for side in (0, 1):
            ab_copy(sec, side).wait_send()
            for c in range(sec, CH):
                x_copy(sec, side, c).wait_send()


def finish(u, k, edge, far_x, far_ab, step, out_state, out_register, done, sem):
    inner = [
        pltpu.make_async_copy(
            src.at[:, pl.ds(1, NX - 2)], dst.at[:, pl.ds(1, NX - 2)], sem.at[i, 0]
        )
        for i, (src, dst) in enumerate(((u, out_state), (k, out_register)))
    ]
    for copy in inner:
        copy.start()
    outer = []
    for side in (0, 1):
        x = 0 if side == 0 else NX - 1
        for c in range(CH):
            rows = pl.ds(ROWS * c, ROWS)
            own = [u[v, x, rows, :] for v in range(NV)]
            if c:
                far = [far_x[side, c - 1, v] for v in range(NV)]
            else:
                far = [far_ab[0, side, v] + step[...] * far_ab[1, side, v] for v in range(NV)]
            extra = x_face(side, own, far)
            for v in range(NV):
                new_k, new_u = advance(
                    1, k[v, x, rows, :], own[v], step[...], edge[side, v, rows, :] + extra[v]
                )
                done[0, side, v, rows, :] = new_u
                done[1, side, v, rows, :] = new_k
        for i, dst in enumerate((out_state, out_register)):
            copy = pltpu.make_async_copy(done.at[i, side], dst.at[:, x], sem.at[i, 1 + side])
            copy.start()
            outer.append(copy)
    for copy in inner + outer:
        copy.wait()


def shards(sizes, state, register):
    mat_z, mat_y = operators()
    nz, nxl, ny, nxh, nco = sizes
    steps_1, steps_2 = z_steps(nz)
    counts = (len(steps_1), len(steps_2) * nxh * nxl * nco - 1, ny - 1)
    block = (NV, NX, NY, NZ)
    vmem = lambda *shape: pltpu.VMEM(shape, jnp.float32)
    dma = lambda *shape: pltpu.SemaphoreType.DMA(shape)
    array = lambda *shape: jax.ShapeDtypeStruct(shape, jnp.float32)
    in_vmem = pl.BlockSpec(memory_space=pltpu.VMEM)
    in_hbm = pl.BlockSpec(memory_space=pltpu.HBM)
    parts = pl.pallas_call(
        functools.partial(kernel, sizes),
        out_shape=(
            array(*block),
            array(*block),
            array(2, NV, NY, NZ),
            array(2, CH - 1, NV, ROWS, NZ),
            array(2, 2, NV, ROWS, NZ),
            array(ROWS, NZ),
        ),
        in_specs=[in_hbm] * 4,
        out_specs=[in_vmem] * 6,
        scratch_shapes=[
            vmem(*block),
            vmem(*block),
            vmem(*block),
            vmem(*block),
            pltpu.VMEM((2, 2, 2 * LANES, 2 * LANES), jnp.bfloat16),
            pltpu.VMEM((2, NX * NY, NX * NY), jnp.bfloat16),
            vmem(ROWS, NZ),
            vmem(3, 1, LANES),
            vmem(counts[0], 1, LANES),
            vmem(counts[1], 1, LANES),
            vmem(counts[2], 1, LANES),
            vmem(2, 2, NV, ROWS, NZ),
            vmem(2, 2, NY, LANES),
            vmem(2, 2, NV, ROWS, NZ),
            vmem(2, 2, NY, LANES),
            vmem(2, CH, NV, ROWS, NZ),
            vmem(2, 2, NV, ROWS, NZ),
            vmem(2, NV, ROWS, NZ),
            vmem(2, NV, NY, LANES),
            dma(NX + 3),
            dma(2, 2, CH),
            dma(2, 2, CH),
            dma(2, 2),
            dma(2, 2),
            dma(2, 2, 2),
            dma(2, 2, 2),
            dma(sum(counts)),
            dma(sum(counts)),
        ],
        compiler_params=pltpu.CompilerParams(
            collective_id=0, has_side_effects=True, vmem_limit_bytes=32 * 2**20
        ),
        name="sections",
    )(*[pltpu.with_memory_space_constraint(x, pltpu.HBM) for x in (state, register, mat_z, mat_y)])
    return pl.pallas_call(
        finish,
        out_shape=(array(*block), array(*block)),
        in_specs=[in_vmem] * 6,
        out_specs=[in_hbm] * 2,
        scratch_shapes=[vmem(2, 2, NV, NY, NZ), dma(2, 3)],
        compiler_params=pltpu.CompilerParams(vmem_limit_bytes=16 * 2**20),
        name="finish",
    )(*parts)


def solution(mesh):
    gx, gy, gz = (mesh.shape[a] for a in ("gx", "gy", "gz"))
    sizes = (gx // 2, 2, gy, gz // 2, 2)
    torus = Mesh(mesh.devices.reshape(sizes), AXES)
    placed = P(None, ("gx_0", "gx_1"), "gy", ("gz_0", "gz_1"))
    return jax.shard_map(
        functools.partial(shards, sizes),
        mesh=torus,
        in_specs=(placed, placed),
        out_specs=(placed, placed),
        check_vma=False,
    )
```

```python
import functools
import math

import jax
import jax.numpy as jnp
import numpy as np
from jax import lax
from jax.experimental import pallas as pl
from jax.experimental.pallas import tpu as pltpu
from jax.sharding import Mesh
from jax.sharding import PartitionSpec as P

AXES = ("gx_0", "gx_1", "gy", "gz_0", "gz_1")
MESH = pl.DeviceIdType.MESH

GAMMA = 1.4
GM1 = 0.4
ELEM_WIDTH = 0.05
COURANT = 0.5
COEFFS = (
    (-567301805773.0 / 1357537059087.0, 5161836677717.0 / 13612068292357.0),
    (-2404267990393.0 / 2016746695238.0, 1720146321549.0 / 2090206949498.0),
)
NV = 5
N = 6
NX, NY, NZ = 6, 24, 384
ROWS = 8
CH = NY // ROWS
LANES = 128
AHEAD = 2 * LANES
SCALE = 2.0 / ELEM_WIDTH
FACE = SCALE * 15.0 * 0.5


def gll_derivative():
    seven = math.sqrt(7.0)
    inner = math.sqrt(1.0 / 3.0 - 2.0 * seven / 21.0)
    outer = math.sqrt(1.0 / 3.0 + 2.0 * seven / 21.0)
    points = np.array([-1.0, -outer, -inner, inner, outer, 1.0])
    count = len(points)
    weights = np.array(
        [np.prod([points[i] - points[j] for j in range(count) if j != i]) for i in range(count)]
    )
    table = np.zeros((count, count))
    for i in range(count):
        for j in range(count):
            if i != j:
                table[i, j] = weights[i] / weights[j] / (points[i] - points[j])
        table[i, i] = -np.sum(table[i])
    return table


DIFF = gll_derivative()


def line_operator(length):
    elems = length // N
    op = np.kron(np.eye(elems), -SCALE * DIFF)
    for e in range(elems - 1):
        last, first = N * e + N - 1, N * e + N
        for row in (last, first):
            op[row, last] += FACE
            op[row, first] -= FACE
    return op


def halves(x):
    top = x.astype(jnp.bfloat16)
    return top, (x - top.astype(jnp.float32)).astype(jnp.bfloat16)


def operators():
    along_z = line_operator(NZ).T
    cut = 2 * LANES - (2 * LANES) % N
    low = along_z[: 2 * LANES, : 2 * LANES].copy()
    low[:, cut:] = 0.0
    high = along_z[LANES:, LANES:].copy()
    high[:, : cut - LANES] = 0.0
    along_y = np.kron(np.eye(NX), line_operator(NY))
    return tuple(jnp.stack(halves(jnp.asarray(m, jnp.float32))) for m in (np.stack([low, high]), along_y))


def z_steps(nz):
    assert nz <= 8
    return (
        sorted({i % nz for i in (1, -1, 2, -2)} - {0}),
        sorted({i % nz for i in (0, 2, -2)}),
    )


def primitives(u):
    inv = 1.0 / u[0]
    vel = [u[1] * inv, u[2] * inv, u[3] * inv]
    press = GM1 * (u[4] - 0.5 * (u[1] * vel[0] + u[2] * vel[1] + u[3] * vel[2]))
    sound = jnp.sqrt(GAMMA * press * inv)
    return vel, press, sound


def flux(u, vel, press, d):
    parts = [u[1 + d], u[1] * vel[d], u[2] * vel[d], u[3] * vel[d], (u[4] + press) * vel[d]]
    parts[1 + d] = parts[1 + d] + press
    return parts


def face_terms(left, right, d):
    vel_l, press_l, sound_l = primitives(left)
    vel_r, press_r, sound_r = primitives(right)
    flux_l = flux(left, vel_l, press_l, d)
    flux_r = flux(right, vel_r, press_r, d)
    lam = FACE * jnp.maximum(jnp.abs(vel_l[d]) + sound_l, jnp.abs(vel_r[d]) + sound_r)
    a = [FACE * (fl - fr) for fl, fr in zip(flux_l, flux_r)]
    b = [lam * (r - l) for l, r in zip(left, right)]
    return a, b


def x_face(side, own, far):
    a, b = face_terms(far, own, 0) if side == 0 else face_terms(own, far, 0)
    return [p - q if side == 0 else p + q for p, q in zip(a, b)]


def advance(sec, k, u, dt, r):
    a, b = COEFFS[sec]
    new_k = a * k + dt * r
    return new_k, u + b * new_k


def kernel(
    sizes,
    state,
    register,
    mat_z,
    mat_y,
    u,
    k,
    edge,
    far_x,
    far_rest,
    far_ab,
    step,
    res,
    fx,
    fy,
    fz,
    mz,
    my,
    mask_z,
    top,
    top_1,
    top_2,
    top_3,
    y_pack,
    z_pack,
    y_halo,
    z_halo,
    near_x,
    ab,
    y_corr,
    z_corr,
    load_sem,
    send_x,
    recv_x,
    send_ab,
    recv_ab,
    send_yz,
    recv_yz,
    send_top,
    recv_top,
):
    nz, nxl, ny, nxh, nco = sizes
    z, xl, y, xh, co = (lax.axis_index(a) for a in AXES)

    def device(z_=z, xl_=xl, y_=y, xh_=xh, co_=co):
        return dict(zip(AXES, (z_, xl_, y_, xh_, co_)))

    def wrap(i, n):
        return lax.rem(i + n, n)

    other_xl, other_co = wrap(xl + 1, nxl), wrap(co + 1, nco)
    gx = (
        device(z_=wrap(z + xl - 1, nz), xl_=other_xl),
        device(z_=wrap(z + xl, nz), xl_=other_xl),
    )
    gy = (device(y_=wrap(y - 1, ny)), device(y_=wrap(y + 1, ny)))
    gz = (
        device(xh_=wrap(xh + co - 1, nxh), co_=other_co),
        device(xh_=wrap(xh + co, nxh), co_=other_co),
    )
    def at(i, a, b, c):
        return device(
            z_=wrap(z + i, nz), xh_=wrap(xh + a, nxh), xl_=wrap(xl + b, nxl), co_=wrap(co + c, nco)
        )

    steps_1, steps_2 = z_steps(nz)
    group_1 = [device(z_=wrap(z + i, nz)) for i in steps_1]
    group_2 = [
        at(i, a, b, c)
        for i in steps_2
        for a in range(nxh)
        for b in range(nxl)
        for c in range(nco)
        if i or a or b or c
    ]
    group_3 = [device(y_=wrap(y + i, ny)) for i in range(1, ny)]
    group_x = [
        at(0, a, b, c) for a in range(nxh) for b in range(nxl) for c in range(nco) if a or b or c
    ]
    diagonal = device(z_=wrap(z + 2 * xl - 1, nz), xl_=other_xl)

    loads = [
        pltpu.make_async_copy(mat_z, mz, load_sem.at[NX]),
        pltpu.make_async_copy(mat_y, my, load_sem.at[NX + 1]),
        pltpu.make_async_copy(register, k, load_sem.at[NX + 2]),
    ]

    def load_plane(x):
        return pltpu.make_async_copy(state.at[:, x], u.at[:, x], load_sem.at[x])

    for x in range(NX):
        load_plane(x).start()
    for load in loads:
        load.start()
    barrier = pltpu.get_barrier_semaphore()
    partners = group_1 + group_x + group_3 + [diagonal]
    for partner in partners:
        pl.semaphore_signal(barrier, inc=1, device_id=partner, device_id_type=MESH)

    lane = lax.broadcasted_iota(jnp.int32, (ROWS, NZ), 1)
    lane_f = lane.astype(jnp.float32)
    place = lane_f - N * jnp.floor((lane_f + 0.5) * (1.0 / N))
    mask_z[...] = jnp.where((place > N - 1.5) & (lane < NZ - 1), FACE, 0.0)
    row = lax.broadcasted_iota(jnp.int32, (ROWS, NZ), 0)
    lane_1 = lax.broadcasted_iota(jnp.int32, (NY, LANES), 1)

    def chunk(ref, x, c):
        return [ref[v, x, pl.ds(ROWS * c, ROWS), :] for v in range(NV)]

    def speed_body(x, carry):
        load_plane(x).wait()
        for c in range(CH):
            w = chunk(u, x, c)
            vel, press, sound = primitives(w)
            mom = jnp.sqrt(w[1] * w[1] + w[2] * w[2] + w[3] * w[3])
            s = mom * (1.0 / w[0]) + sound
            carry = jnp.maximum(carry, s)
        return carry

    best = lax.fori_loop(0, NX, speed_body, jnp.zeros((ROWS, NZ), jnp.float32))
    best = jnp.maximum(
        jnp.maximum(best[:, :LANES], best[:, LANES : 2 * LANES]), best[:, 2 * LANES :]
    )
    top[0] = jnp.max(best, axis=0, keepdims=True)

    def pack(sec):
        def body(v, carry):
            low, high = carry
            for x in range(NX):
                y_pack[sec, 0, v, x : x + 1, :] = u[v, x, 0:1, :]
                y_pack[sec, 1, v, x : x + 1, :] = u[v, x, NY - 1 : NY, :]
                here = lane_1 == v * NX + x
                low = jnp.where(here, u[v, x, :, 0:LANES][:, 0:1], low)
                high = jnp.where(here, u[v, x, :, NZ - LANES : NZ][:, LANES - 1 : LANES], high)
            for x in range(NX, ROWS):
                y_pack[sec, 0, v, x : x + 1, :] = u[v, 0, 0:1, :]
                y_pack[sec, 1, v, x : x + 1, :] = u[v, 0, NY - 1 : NY, :]
            return low, high

        ones = jnp.ones((NY, LANES), jnp.float32)
        low, high = lax.fori_loop(0, NV, body, (ones, ones), unroll=True)
        z_pack[sec, 0] = low
        z_pack[sec, 1] = high

    def remote(src, dst, send, recv, to):
        return pltpu.make_async_remote_copy(
            src_ref=src,
            dst_ref=dst,
            send_sem=send,
            recv_sem=recv,
            device_id=to,
            device_id_type=MESH,
        )

    def plane(side):
        return 0 if side == 0 else NX - 1

    def x_copy(sec, side, c):
        lanes = pl.ds(AHEAD, NZ - AHEAD) if sec and c == 0 else pl.ds(0, NZ)
        slots = near_x.at[1 - side, c]
        if sec:
            slots = far_x.at[1 - side, c - 1] if c else far_rest.at[1 - side]
        return remote(
            (u if sec else state).at[:, plane(side), pl.ds(ROWS * c, ROWS), lanes],
            slots,
            send_x.at[sec, side, c],
            recv_x.at[sec, 1 - side, c],
            gx[side],
        )

    def ab_copy(part, side):
        return remote(
            ab.at[part, side],
            far_ab.at[part, 1 - side],
            send_ab.at[part, side],
            recv_ab.at[part, 1 - side],
            gx[side],
        )

    def y_copy(sec, side):
        return remote(
            y_pack.at[sec, side],
            y_halo.at[sec, 1 - side],
            send_yz.at[sec, 0, side],
            recv_yz.at[sec, 0, 1 - side],
            gy[side],
        )

    def z_copy(sec, side):
        return remote(
            z_pack.at[sec, side],
            z_halo.at[sec, 1 - side],
            send_yz.at[sec, 1, side],
            recv_yz.at[sec, 1, 1 - side],
            gz[side],
        )

    def top_copies(stage, group, slots, first):
        return [
            remote(top.at[stage], slots.at[i], send_top.at[first + i], recv_top.at[first + i], to)
            for i, to in enumerate(group)
        ]

    tops_1 = top_copies(0, group_1, top_1, 0)
    tops_2 = top_copies(1, group_2, top_2, len(group_1))
    tops_3 = top_copies(2, group_3, top_3, len(group_1) + len(group_2))

    def start(copies):
        for copy in copies:
            copy.start()

    def gather_top(stage, copies, slots):
        value = top[stage]
        for i, copy in enumerate(copies):
            copy.wait_recv()
            value = jnp.maximum(value, slots[i])
        return value

    def y_z_copies(sec):
        return [z_copy(sec, 0), z_copy(sec, 1), y_copy(sec, 0), y_copy(sec, 1)]

    def fluxes_and_jumps():
        def body(x, carry):
            for c in range(CH):
                w = chunk(u, x, c)
                vel, press, sound = primitives(w)
                rows = pl.ds(ROWS * c, ROWS)
                for d, to in enumerate((fx, fy, fz)):
                    for v, part in enumerate(flux(w, vel, press, d)):
                        to[v, x, rows, :] = part
                s_y = jnp.abs(vel[1]) + sound
                s_z = jnp.abs(vel[2]) + sound
                lam_y = jnp.where(
                    row == N - 1 - 2 * c,
                    FACE * jnp.maximum(s_y, pltpu.roll(s_y, ROWS - 1, 0)),
                    0.0,
                )
                lam_z = mask_z[...] * jnp.maximum(s_z, pltpu.roll(s_z, NZ - 1, 1))
                for v in range(NV):
                    t_y = lam_y * (pltpu.roll(w[v], ROWS - 1, 0) - w[v])
                    t_z = lam_z * (pltpu.roll(w[v], NZ - 1, 1) - w[v])
                    res[v, x, rows, :] = (t_y - pltpu.roll(t_y, 1, 0)) + (
                        t_z - pltpu.roll(t_z, 1, 1)
                    )
            return carry

        lax.fori_loop(0, NX, body, 0)

    def dot(a, b):
        (a_top, a_rest), (b_top, b_rest) = a, b
        one = lambda p, q: jnp.dot(p, q, preferred_element_type=jnp.float32)
        return one(a_top, b_top) + (one(a_top, b_rest) + one(a_rest, b_top))

    def lines_y_z():
        def body(v, carry):
            along_z = halves(fz[v].reshape(NX * NY, NZ))
            low = dot([p[:, : 2 * LANES] for p in along_z], (mz[0, 0], mz[1, 0]))
            high = dot([p[:, LANES:] for p in along_z], (mz[0, 1], mz[1, 1]))
            both = jnp.concatenate(
                [low[:, :LANES], low[:, LANES:] + high[:, :LANES], high[:, LANES:]], axis=1
            )
            along_y = dot((my[0], my[1]), halves(fy[v].reshape(NX * NY, NZ)))
            res[v] = res[v] + (both + along_y).reshape(NX, NY, NZ)
            return carry

        lax.fori_loop(0, NV, body, 0, unroll=True)

    def lines_x():
        half = N // 2
        even = [[-SCALE * 0.5 * (DIFF[i, j] + DIFF[i, N - 1 - j]) for j in range(half)] for i in range(half)]
        odd = [[-SCALE * 0.5 * (DIFF[i, j] - DIFF[i, N - 1 - j]) for j in range(half)] for i in range(half)]

        def body(v, carry):
            for c in range(CH):
                rows = pl.ds(ROWS * c, ROWS)
                f = [fx[v, x, rows, :] for x in range(NX)]
                plus = [f[j] + f[N - 1 - j] for j in range(half)]
                minus = [f[j] - f[N - 1 - j] for j in range(half)]
                for i in range(half):
                    a = sum(even[i][j] * plus[j] for j in range(half))
                    b = sum(odd[i][j] * minus[j] for j in range(half))
                    res[v, i, rows, :] += b + a
                    res[v, N - 1 - i, rows, :] += b - a
            return carry

        lax.fori_loop(0, NV, body, 0, unroll=True)

    def y_z_faces(sec):
        for side in (0, 1):
            y_copy(sec, 1 - side).wait_recv()
            own = [y_pack[sec, side, v] for v in range(NV)]
            far = [y_halo[sec, side, v] for v in range(NV)]
            a, b = face_terms(far, own, 1) if side == 0 else face_terms(own, far, 1)
            for v in range(NV):
                y_corr[side, v] = a[v] - b[v] if side == 0 else a[v] + b[v]
            z_copy(sec, 1 - side).wait_recv()

            def part(ref, v):
                tile = ref[sec, side]
                return tile if v == 0 else pltpu.roll(tile, LANES - NX * v, 1)

            own = [part(z_pack, v) for v in range(NV)]
            far = [part(z_halo, v) for v in range(NV)]
            a, b = face_terms(far, own, 2) if side == 0 else face_terms(own, far, 2)
            for v in range(NV):
                z_corr[side, v] = a[v] - b[v] if side == 0 else a[v] + b[v]

        def body(v, carry):
            for x in range(NX):
                res[v, x, 0:1, :] += y_corr[0, v, x : x + 1, :]
                res[v, x, NY - 1 : NY, :] += y_corr[1, v, x : x + 1, :]
                low = z_corr[0, v][:, x : x + 1]
                high = z_corr[1, v][:, x : x + 1]
                res[v, x, :, 0:LANES] += jnp.where(lane_1 == 0, low, 0.0)
                res[v, x, :, NZ - LANES : NZ] += jnp.where(lane_1 == LANES - 1, high, 0.0)
            return carry

        lax.fori_loop(0, NV, body, 0, unroll=True)

    def update(sec, x, c, extra):
        rows = pl.ds(ROWS * c, ROWS)
        for v in range(NV):
            r = res[v, x, rows, :]
            if extra is not None:
                r = r + extra[v]
            new_k, new_u = advance(sec, k[v, x, rows, :], u[v, x, rows, :], step[...], r)
            k[v, x, rows, :] = new_k
            u[v, x, rows, :] = new_u

    def known_part(side):
        a, b = COEFFS[0]
        rows = pl.ds(0, ROWS)
        for v in range(NV):
            ab[0, side, v] = u[v, plane(side), rows, 0:AHEAD] + b * (
                a * k[v, plane(side), rows, 0:AHEAD]
            )
        ab_copy(0, side).start()

    def step_part(side):
        extra = boundary_terms(side, 0)
        for v in range(NV):
            r = res[v, plane(side), 0:ROWS, :] + extra[v]
            res[v, plane(side), 0:ROWS, :] = r
            ab[1, side, v] = COEFFS[0][1] * r[:, :AHEAD]
        ab_copy(1, side).start()

    def boundary_terms(side, c):
        x_copy(0, 1 - side, c).wait_recv()
        return x_face(side, chunk(u, plane(side), c), [near_x[side, c, v] for v in range(NV)])

    def update_interior(sec):
        def body(x, carry):
            for c in range(CH):
                update(sec, x, c, None)
            return carry

        lax.fori_loop(1, NX - 1, body, 0)

    pl.semaphore_wait(barrier, len(partners))
    start(tops_1)
    start([x_copy(0, 0, 0), x_copy(0, 1, 0)])
    pack(0)
    start(y_z_copies(0))
    fluxes_and_jumps()
    top[1] = gather_top(0, tops_1, top_1)
    start(tops_2)
    for c in range(1, CH):
        start([x_copy(0, 0, c), x_copy(0, 1, c)])
    loads[2].wait()
    for side in (0, 1):
        known_part(side)
    loads[0].wait()
    loads[1].wait()
    lines_y_z()
    top[2] = gather_top(1, tops_2, top_2)
    start(tops_3)
    lines_x()
    y_z_faces(0)
    for side in (0, 1):
        step_part(side)
    value = gather_top(2, tops_3, top_3)
    value = jnp.max(jnp.broadcast_to(value, (ROWS, LANES)), axis=1, keepdims=True)
    step[...] = jnp.broadcast_to(COURANT * ELEM_WIDTH / (11.0 * value), (ROWS, NZ))

    for c in (1, 0, *range(2, CH)):
        for side in (0, 1):
            update(0, plane(side), c, boundary_terms(side, c) if c else None)
            if c < CH - 1:
                x_copy(1, side, c).start()
    update_interior(0)
    pack(1)
    start(y_z_copies(1))
    start([x_copy(1, 0, CH - 1), x_copy(1, 1, CH - 1)])

    fluxes_and_jumps()
    lines_y_z()
    lines_x()
    y_z_faces(1)
    update_interior(1)
    for v in range(NV):
        edge[0, v] = res[v, 0]
        edge[1, v] = res[v, NX - 1]
    for side in (0, 1):
        for part in (0, 1):
            ab_copy(part, side).wait_recv()
        for c in range(CH):
            x_copy(1, side, c).wait_recv()

    for copy in tops_1 + tops_2 + tops_3:
        copy.wait_send()
    for sec in (0, 1):
        for copy in y_z_copies(sec):
            copy.wait_send()
        for side in (0, 1):
            ab_copy(sec, side).wait_send()
            for c in range(CH):
                x_copy(sec, side, c).wait_send()


def finish(u, k, edge, far_x, far_rest, far_ab, step, out_state, out_register, done, sem):
    inner = [
        pltpu.make_async_copy(
            src.at[:, pl.ds(1, NX - 2)], dst.at[:, pl.ds(1, NX - 2)], sem.at[i, 0]
        )
        for i, (src, dst) in enumerate(((u, out_state), (k, out_register)))
    ]
    for copy in inner:
        copy.start()
    outer = []
    for side in (0, 1):
        x = 0 if side == 0 else NX - 1
        for c in range(CH):
            rows = pl.ds(ROWS * c, ROWS)
            own = [u[v, x, rows, :] for v in range(NV)]
            if c:
                far = [far_x[side, c - 1, v] for v in range(NV)]
            else:
                dt = step[:, 0:AHEAD]
                far = [
                    jnp.concatenate(
                        [far_ab[0, side, v] + dt * far_ab[1, side, v], far_rest[side, v]], axis=1
                    )
                    for v in range(NV)
                ]
            extra = x_face(side, own, far)
            for v in range(NV):
                new_k, new_u = advance(
                    1, k[v, x, rows, :], own[v], step[...], edge[side, v, rows, :] + extra[v]
                )
                done[0, side, v, rows, :] = new_u
                done[1, side, v, rows, :] = new_k
        for i, dst in enumerate((out_state, out_register)):
            copy = pltpu.make_async_copy(done.at[i, side], dst.at[:, x], sem.at[i, 1 + side])
            copy.start()
            outer.append(copy)
    for copy in inner + outer:
        copy.wait()


def shards(sizes, state, register):
    mat_z, mat_y = operators()
    nz, nxl, ny, nxh, nco = sizes
    steps_1, steps_2 = z_steps(nz)
    counts = (len(steps_1), len(steps_2) * nxh * nxl * nco - 1, ny - 1)
    block = (NV, NX, NY, NZ)
    vmem = lambda *shape: pltpu.VMEM(shape, jnp.float32)
    dma = lambda *shape: pltpu.SemaphoreType.DMA(shape)
    array = lambda *shape: jax.ShapeDtypeStruct(shape, jnp.float32)
    in_vmem = pl.BlockSpec(memory_space=pltpu.VMEM)
    in_hbm = pl.BlockSpec(memory_space=pltpu.HBM)
    parts = pl.pallas_call(
        functools.partial(kernel, sizes),
        out_shape=(
            array(*block),
            array(*block),
            array(2, NV, NY, NZ),
            array(2, CH - 1, NV, ROWS, NZ),
            array(2, NV, ROWS, NZ - AHEAD),
            array(2, 2, NV, ROWS, AHEAD),
            array(ROWS, NZ),
        ),
        in_specs=[in_hbm] * 4,
        out_specs=[in_vmem] * 7,
        scratch_shapes=[
            vmem(*block),
            vmem(*block),
            vmem(*block),
            vmem(*block),
            pltpu.VMEM((2, 2, 2 * LANES, 2 * LANES), jnp.bfloat16),
            pltpu.VMEM((2, NX * NY, NX * NY), jnp.bfloat16),
            vmem(ROWS, NZ),
            vmem(3, 1, LANES),
            vmem(counts[0], 1, LANES),
            vmem(counts[1], 1, LANES),
            vmem(counts[2], 1, LANES),
            vmem(2, 2, NV, ROWS, NZ),
            vmem(2, 2, NY, LANES),
            vmem(2, 2, NV, ROWS, NZ),
            vmem(2, 2, NY, LANES),
            vmem(2, CH, NV, ROWS, NZ),
            vmem(2, 2, NV, ROWS, AHEAD),
            vmem(2, NV, ROWS, NZ),
            vmem(2, NV, NY, LANES),
            dma(NX + 3),
            dma(2, 2, CH),
            dma(2, 2, CH),
            dma(2, 2),
            dma(2, 2),
            dma(2, 2, 2),
            dma(2, 2, 2),
            dma(sum(counts)),
            dma(sum(counts)),
        ],
        compiler_params=pltpu.CompilerParams(
            collective_id=0, has_side_effects=True, vmem_limit_bytes=32 * 2**20
        ),
        name="sections",
    )(*[pltpu.with_memory_space_constraint(x, pltpu.HBM) for x in (state, register, mat_z, mat_y)])
    return pl.pallas_call(
        finish,
        out_shape=(array(*block), array(*block)),
        in_specs=[in_vmem] * 7,
        out_specs=[in_hbm] * 2,
        scratch_shapes=[vmem(2, 2, NV, NY, NZ), dma(2, 3)],
        compiler_params=pltpu.CompilerParams(vmem_limit_bytes=16 * 2**20),
        name="finish",
    )(*parts)


def solution(mesh):
    gx, gy, gz = (mesh.shape[a] for a in ("gx", "gy", "gz"))
    sizes = (gx // 2, 2, gy, gz // 2, 2)
    torus = Mesh(mesh.devices.reshape(sizes), AXES)
    placed = P(None, ("gx_0", "gx_1"), "gy", ("gz_0", "gz_1"))
    return jax.shard_map(
        functools.partial(shards, sizes),
        mesh=torus,
        in_specs=(placed, placed),
        out_specs=(placed, placed),
        check_vma=False,
    )
```

```python
import functools
import math

import jax
import jax.numpy as jnp
import numpy as np
from jax import lax
from jax.experimental import pallas as pl
from jax.experimental.pallas import tpu as pltpu
from jax.sharding import Mesh
from jax.sharding import PartitionSpec as P

AXES = ("gx_0", "gx_1", "gy", "gz_0", "gz_1")
MESH = pl.DeviceIdType.MESH

GAMMA = 1.4
GM1 = 0.4
ELEM_WIDTH = 0.05
COURANT = 0.5
COEFFS = (
    (-567301805773.0 / 1357537059087.0, 5161836677717.0 / 13612068292357.0),
    (-2404267990393.0 / 2016746695238.0, 1720146321549.0 / 2090206949498.0),
)
NV = 5
N = 6
NX, NY, NZ = 6, 24, 384
ROWS = 8
CH = NY // ROWS
LANES = 128
AHEAD = 2 * LANES
SCALE = 2.0 / ELEM_WIDTH
FACE = SCALE * 15.0 * 0.5


def gll_derivative():
    seven = math.sqrt(7.0)
    inner = math.sqrt(1.0 / 3.0 - 2.0 * seven / 21.0)
    outer = math.sqrt(1.0 / 3.0 + 2.0 * seven / 21.0)
    points = np.array([-1.0, -outer, -inner, inner, outer, 1.0])
    count = len(points)
    weights = np.array(
        [np.prod([points[i] - points[j] for j in range(count) if j != i]) for i in range(count)]
    )
    table = np.zeros((count, count))
    for i in range(count):
        for j in range(count):
            if i != j:
                table[i, j] = weights[i] / weights[j] / (points[i] - points[j])
        table[i, i] = -np.sum(table[i])
    return table


DIFF = gll_derivative()


def line_operator(length):
    elems = length // N
    op = np.kron(np.eye(elems), -SCALE * DIFF)
    for e in range(elems - 1):
        last, first = N * e + N - 1, N * e + N
        for row in (last, first):
            op[row, last] += FACE
            op[row, first] -= FACE
    return op


def halves(x):
    top = x.astype(jnp.bfloat16)
    return top, (x - top.astype(jnp.float32)).astype(jnp.bfloat16)


def operators():
    along_z = line_operator(NZ).T
    cut = 2 * LANES - (2 * LANES) % N
    low = along_z[: 2 * LANES, : 2 * LANES].copy()
    low[:, cut:] = 0.0
    high = along_z[LANES:, LANES:].copy()
    high[:, : cut - LANES] = 0.0
    along_y = np.kron(np.eye(NX), line_operator(NY))
    return tuple(jnp.stack(halves(jnp.asarray(m, jnp.float32))) for m in (np.stack([low, high]), along_y))


def z_steps(nz):
    assert nz <= 8
    return (
        sorted({i % nz for i in (1, -1, 2, -2)} - {0}),
        sorted({i % nz for i in (0, 2, -2)}),
    )


def primitives(u):
    inv = 1.0 / u[0]
    vel = [u[1] * inv, u[2] * inv, u[3] * inv]
    press = GM1 * (u[4] - 0.5 * (u[1] * vel[0] + u[2] * vel[1] + u[3] * vel[2]))
    sound = jnp.sqrt(GAMMA * press * inv)
    return vel, press, sound


def flux(u, vel, press, d):
    parts = [u[1 + d], u[1] * vel[d], u[2] * vel[d], u[3] * vel[d], (u[4] + press) * vel[d]]
    parts[1 + d] = parts[1 + d] + press
    return parts


def face_terms(left, right, d):
    vel_l, press_l, sound_l = primitives(left)
    vel_r, press_r, sound_r = primitives(right)
    flux_l = flux(left, vel_l, press_l, d)
    flux_r = flux(right, vel_r, press_r, d)
    lam = FACE * jnp.maximum(jnp.abs(vel_l[d]) + sound_l, jnp.abs(vel_r[d]) + sound_r)
    a = [FACE * (fl - fr) for fl, fr in zip(flux_l, flux_r)]
    b = [lam * (r - l) for l, r in zip(left, right)]
    return a, b


def x_face(side, own, far):
    a, b = face_terms(far, own, 0) if side == 0 else face_terms(own, far, 0)
    return [p - q if side == 0 else p + q for p, q in zip(a, b)]


def advance(sec, k, u, dt, r):
    a, b = COEFFS[sec]
    new_k = a * k + dt * r
    return new_k, u + b * new_k


def kernel(
    sizes,
    state,
    register,
    mat_z,
    mat_y,
    u,
    k,
    edge,
    far_x,
    far_rest,
    far_ab,
    step,
    res,
    fx,
    fy,
    fz,
    mz,
    my,
    mask_z,
    top,
    top_1,
    top_2,
    top_3,
    y_pack,
    z_pack,
    y_halo,
    z_halo,
    near_x,
    ab,
    y_corr,
    z_corr,
    load_sem,
    send_x,
    recv_x,
    send_ab,
    recv_ab,
    send_yz,
    recv_yz,
    send_top,
    recv_top,
):
    nz, nxl, ny, nxh, nco = sizes
    z, xl, y, xh, co = (lax.axis_index(a) for a in AXES)

    def device(z_=z, xl_=xl, y_=y, xh_=xh, co_=co):
        return dict(zip(AXES, (z_, xl_, y_, xh_, co_)))

    def wrap(i, n):
        return lax.rem(i + n, n)

    other_xl, other_co = wrap(xl + 1, nxl), wrap(co + 1, nco)
    gx = (
        device(z_=wrap(z + xl - 1, nz), xl_=other_xl),
        device(z_=wrap(z + xl, nz), xl_=other_xl),
    )
    gy = (device(y_=wrap(y - 1, ny)), device(y_=wrap(y + 1, ny)))
    gz = (
        device(xh_=wrap(xh + co - 1, nxh), co_=other_co),
        device(xh_=wrap(xh + co, nxh), co_=other_co),
    )
    def at(i, a, b, c):
        return device(
            z_=wrap(z + i, nz), xh_=wrap(xh + a, nxh), xl_=wrap(xl + b, nxl), co_=wrap(co + c, nco)
        )

    steps_1, steps_2 = z_steps(nz)
    group_1 = [device(z_=wrap(z + i, nz)) for i in steps_1]
    group_2 = [
        at(i, a, b, c)
        for i in steps_2
        for a in range(nxh)
        for b in range(nxl)
        for c in range(nco)
        if i or a or b or c
    ]
    group_3 = [device(y_=wrap(y + i, ny)) for i in range(1, ny)]
    group_x = [
        at(0, a, b, c) for a in range(nxh) for b in range(nxl) for c in range(nco) if a or b or c
    ]
    diagonal = device(z_=wrap(z + 2 * xl - 1, nz), xl_=other_xl)

    loads = [
        pltpu.make_async_copy(mat_z, mz, load_sem.at[NX]),
        pltpu.make_async_copy(mat_y, my, load_sem.at[NX + 1]),
        pltpu.make_async_copy(register, k, load_sem.at[NX + 2]),
    ]

    def load_plane(x):
        return pltpu.make_async_copy(state.at[:, x], u.at[:, x], load_sem.at[x])

    for x in range(NX):
        load_plane(x).start()
    for load in loads:
        load.start()
    barrier = pltpu.get_barrier_semaphore()
    partners = group_1 + group_x + group_3 + [diagonal]
    for partner in partners:
        pl.semaphore_signal(barrier, inc=1, device_id=partner, device_id_type=MESH)

    lane = lax.broadcasted_iota(jnp.int32, (ROWS, NZ), 1)
    lane_f = lane.astype(jnp.float32)
    place = lane_f - N * jnp.floor((lane_f + 0.5) * (1.0 / N))
    mask_z[...] = jnp.where((place > N - 1.5) & (lane < NZ - 1), FACE, 0.0)
    row = lax.broadcasted_iota(jnp.int32, (ROWS, NZ), 0)
    lane_1 = lax.broadcasted_iota(jnp.int32, (NY, LANES), 1)

    def chunk(ref, x, c):
        return [ref[v, x, pl.ds(ROWS * c, ROWS), :] for v in range(NV)]

    def speed_body(x, carry):
        load_plane(x).wait()
        for c in range(CH):
            w = chunk(u, x, c)
            vel, press, sound = primitives(w)
            mom = jnp.sqrt(w[1] * w[1] + w[2] * w[2] + w[3] * w[3])
            s = mom * (1.0 / w[0]) + sound
            carry = jnp.maximum(carry, s)
        return carry

    best = lax.fori_loop(0, NX, speed_body, jnp.zeros((ROWS, NZ), jnp.float32))
    best = jnp.maximum(
        jnp.maximum(best[:, :LANES], best[:, LANES : 2 * LANES]), best[:, 2 * LANES :]
    )
    top[0] = jnp.max(best, axis=0, keepdims=True)

    def pack(sec):
        def body(v, carry):
            low, high = carry
            for x in range(NX):
                y_pack[sec, 0, v, x : x + 1, :] = u[v, x, 0:1, :]
                y_pack[sec, 1, v, x : x + 1, :] = u[v, x, NY - 1 : NY, :]
                here = lane_1 == v * NX + x
                low = jnp.where(here, u[v, x, :, 0:LANES][:, 0:1], low)
                high = jnp.where(here, u[v, x, :, NZ - LANES : NZ][:, LANES - 1 : LANES], high)
            for x in range(NX, ROWS):
                y_pack[sec, 0, v, x : x + 1, :] = u[v, 0, 0:1, :]
                y_pack[sec, 1, v, x : x + 1, :] = u[v, 0, NY - 1 : NY, :]
            return low, high

        ones = jnp.ones((NY, LANES), jnp.float32)
        low, high = lax.fori_loop(0, NV, body, (ones, ones), unroll=True)
        z_pack[sec, 0] = low
        z_pack[sec, 1] = high

    def remote(src, dst, send, recv, to):
        return pltpu.make_async_remote_copy(
            src_ref=src,
            dst_ref=dst,
            send_sem=send,
            recv_sem=recv,
            device_id=to,
            device_id_type=MESH,
        )

    def plane(side):
        return 0 if side == 0 else NX - 1

    def x_copy(sec, side, c):
        lanes = pl.ds(AHEAD, NZ - AHEAD) if sec and c == 0 else pl.ds(0, NZ)
        slots = near_x.at[1 - side, c]
        if sec:
            slots = far_x.at[1 - side, c - 1] if c else far_rest.at[1 - side]
        return remote(
            (u if sec else state).at[:, plane(side), pl.ds(ROWS * c, ROWS), lanes],
            slots,
            send_x.at[sec, side, c],
            recv_x.at[sec, 1 - side, c],
            gx[side],
        )

    def ab_copy(part, side):
        return remote(
            ab.at[part, side],
            far_ab.at[part, 1 - side],
            send_ab.at[part, side],
            recv_ab.at[part, 1 - side],
            gx[side],
        )

    def y_copy(sec, side):
        return remote(
            y_pack.at[sec, side],
            y_halo.at[sec, 1 - side],
            send_yz.at[sec, 0, side],
            recv_yz.at[sec, 0, 1 - side],
            gy[side],
        )

    def z_copy(sec, side):
        return remote(
            z_pack.at[sec, side],
            z_halo.at[sec, 1 - side],
            send_yz.at[sec, 1, side],
            recv_yz.at[sec, 1, 1 - side],
            gz[side],
        )

    def top_copies(stage, group, slots, first):
        return [
            remote(top.at[stage], slots.at[i], send_top.at[first + i], recv_top.at[first + i], to)
            for i, to in enumerate(group)
        ]

    tops_1 = top_copies(0, group_1, top_1, 0)
    tops_2 = top_copies(1, group_2, top_2, len(group_1))
    tops_3 = top_copies(2, group_3, top_3, len(group_1) + len(group_2))

    def start(copies):
        for copy in copies:
            copy.start()

    def gather_top(stage, copies, slots):
        value = top[stage]
        for i, copy in enumerate(copies):
            copy.wait_recv()
            value = jnp.maximum(value, slots[i])
        return value

    def y_z_copies(sec):
        return [z_copy(sec, 0), z_copy(sec, 1), y_copy(sec, 0), y_copy(sec, 1)]

    def fluxes_and_jumps():
        def body(x, carry):
            for c in range(CH):
                w = chunk(u, x, c)
                vel, press, sound = primitives(w)
                rows = pl.ds(ROWS * c, ROWS)
                for d, to in enumerate((fx, fy, fz)):
                    for v, part in enumerate(flux(w, vel, press, d)):
                        to[v, x, rows, :] = part
                s_y = jnp.abs(vel[1]) + sound
                s_z = jnp.abs(vel[2]) + sound
                lam_y = jnp.where(
                    row == N - 1 - 2 * c,
                    FACE * jnp.maximum(s_y, pltpu.roll(s_y, ROWS - 1, 0)),
                    0.0,
                )
                lam_z = mask_z[...] * jnp.maximum(s_z, pltpu.roll(s_z, NZ - 1, 1))
                for v in range(NV):
                    t_y = lam_y * (pltpu.roll(w[v], ROWS - 1, 0) - w[v])
                    t_z = lam_z * (pltpu.roll(w[v], NZ - 1, 1) - w[v])
                    res[v, x, rows, :] = (t_y - pltpu.roll(t_y, 1, 0)) + (
                        t_z - pltpu.roll(t_z, 1, 1)
                    )
            return carry

        lax.fori_loop(0, NX, body, 0)

    def dot(a, b):
        (a_top, a_rest), (b_top, b_rest) = a, b
        one = lambda p, q: jnp.dot(p, q, preferred_element_type=jnp.float32)
        return one(a_top, b_top) + (one(a_top, b_rest) + one(a_rest, b_top))

    def lines_y_z():
        def body(v, carry):
            along_z = halves(fz[v].reshape(NX * NY, NZ))
            low = dot([p[:, : 2 * LANES] for p in along_z], (mz[0, 0], mz[1, 0]))
            high = dot([p[:, LANES:] for p in along_z], (mz[0, 1], mz[1, 1]))
            both = jnp.concatenate(
                [low[:, :LANES], low[:, LANES:] + high[:, :LANES], high[:, LANES:]], axis=1
            )
            along_y = dot((my[0], my[1]), halves(fy[v].reshape(NX * NY, NZ)))
            res[v] = res[v] + (both + along_y).reshape(NX, NY, NZ)
            return carry

        lax.fori_loop(0, NV, body, 0, unroll=True)

    def lines_x():
        half = N // 2
        even = [[-SCALE * 0.5 * (DIFF[i, j] + DIFF[i, N - 1 - j]) for j in range(half)] for i in range(half)]
        odd = [[-SCALE * 0.5 * (DIFF[i, j] - DIFF[i, N - 1 - j]) for j in range(half)] for i in range(half)]

        def body(v, carry):
            for c in range(CH):
                rows = pl.ds(ROWS * c, ROWS)
                f = [fx[v, x, rows, :] for x in range(NX)]
                plus = [f[j] + f[N - 1 - j] for j in range(half)]
                minus = [f[j] - f[N - 1 - j] for j in range(half)]
                for i in range(half):
                    a = sum(even[i][j] * plus[j] for j in range(half))
                    b = sum(odd[i][j] * minus[j] for j in range(half))
                    res[v, i, rows, :] += b + a
                    res[v, N - 1 - i, rows, :] += b - a
            return carry

        lax.fori_loop(0, NV, body, 0, unroll=True)

    def y_z_faces(sec):
        for side in (0, 1):
            y_copy(sec, 1 - side).wait_recv()
            own = [y_pack[sec, side, v] for v in range(NV)]
            far = [y_halo[sec, side, v] for v in range(NV)]
            a, b = face_terms(far, own, 1) if side == 0 else face_terms(own, far, 1)
            for v in range(NV):
                y_corr[side, v] = a[v] - b[v] if side == 0 else a[v] + b[v]
            z_copy(sec, 1 - side).wait_recv()

            def part(ref, v):
                tile = ref[sec, side]
                return tile if v == 0 else pltpu.roll(tile, LANES - NX * v, 1)

            own = [part(z_pack, v) for v in range(NV)]
            far = [part(z_halo, v) for v in range(NV)]
            a, b = face_terms(far, own, 2) if side == 0 else face_terms(own, far, 2)
            for v in range(NV):
                z_corr[side, v] = a[v] - b[v] if side == 0 else a[v] + b[v]

        def body(v, carry):
            for x in range(NX):
                res[v, x, 0:1, :] += y_corr[0, v, x : x + 1, :]
                res[v, x, NY - 1 : NY, :] += y_corr[1, v, x : x + 1, :]
                low = z_corr[0, v][:, x : x + 1]
                high = z_corr[1, v][:, x : x + 1]
                res[v, x, :, 0:LANES] += jnp.where(lane_1 == 0, low, 0.0)
                res[v, x, :, NZ - LANES : NZ] += jnp.where(lane_1 == LANES - 1, high, 0.0)
            return carry

        lax.fori_loop(0, NV, body, 0, unroll=True)

    def update(sec, x, c, extra):
        rows = pl.ds(ROWS * c, ROWS)
        for v in range(NV):
            r = res[v, x, rows, :]
            if extra is not None:
                r = r + extra[v]
            new_k, new_u = advance(sec, k[v, x, rows, :], u[v, x, rows, :], step[...], r)
            k[v, x, rows, :] = new_k
            u[v, x, rows, :] = new_u

    def known_part(side):
        a, b = COEFFS[0]
        rows = pl.ds(0, ROWS)
        for v in range(NV):
            ab[0, side, v] = u[v, plane(side), rows, 0:AHEAD] + b * (
                a * k[v, plane(side), rows, 0:AHEAD]
            )
        ab_copy(0, side).start()

    def step_part(side):
        extra = boundary_terms(side, 0)
        for v in range(NV):
            r = res[v, plane(side), 0:ROWS, :] + extra[v]
            res[v, plane(side), 0:ROWS, :] = r
            ab[1, side, v] = COEFFS[0][1] * r[:, :AHEAD]
        ab_copy(1, side).start()

    def boundary_terms(side, c):
        x_copy(0, 1 - side, c).wait_recv()
        return x_face(side, chunk(u, plane(side), c), [near_x[side, c, v] for v in range(NV)])

    def update_interior(sec):
        def body(x, carry):
            for c in range(CH):
                update(sec, x, c, None)
            return carry

        lax.fori_loop(1, NX - 1, body, 0)

    pl.semaphore_wait(barrier, len(partners))
    start(tops_1)
    start([x_copy(0, 0, 0), x_copy(0, 1, 0)])
    pack(0)
    start(y_z_copies(0))
    fluxes_and_jumps()
    loads[0].wait()
    loads[1].wait()
    lines_y_z()
    top[1] = gather_top(0, tops_1, top_1)
    start(tops_2)
    for c in range(1, CH):
        start([x_copy(0, 0, c), x_copy(0, 1, c)])
    loads[2].wait()
    for side in (0, 1):
        known_part(side)
    top[2] = gather_top(1, tops_2, top_2)
    start(tops_3)
    lines_x()
    y_z_faces(0)
    for side in (0, 1):
        step_part(side)
    value = gather_top(2, tops_3, top_3)
    value = jnp.max(jnp.broadcast_to(value, (ROWS, LANES)), axis=1, keepdims=True)
    step[...] = jnp.broadcast_to(COURANT * ELEM_WIDTH / (11.0 * value), (ROWS, NZ))

    for c in (1, 0, *range(2, CH)):
        for side in (0, 1):
            update(0, plane(side), c, boundary_terms(side, c) if c else None)
    update_interior(0)
    pack(1)
    start(y_z_copies(1))
    for c in (1, 0, *range(2, CH)):
        start([x_copy(1, 0, c), x_copy(1, 1, c)])

    fluxes_and_jumps()
    lines_y_z()
    lines_x()
    y_z_faces(1)
    update_interior(1)
    for v in range(NV):
        edge[0, v] = res[v, 0]
        edge[1, v] = res[v, NX - 1]
    for side in (0, 1):
        for part in (0, 1):
            ab_copy(part, side).wait_recv()
        for c in range(CH):
            x_copy(1, side, c).wait_recv()

    for copy in tops_1 + tops_2 + tops_3:
        copy.wait_send()
    for sec in (0, 1):
        for copy in y_z_copies(sec):
            copy.wait_send()
        for side in (0, 1):
            ab_copy(sec, side).wait_send()
            for c in range(CH):
                x_copy(sec, side, c).wait_send()


def finish(u, k, edge, far_x, far_rest, far_ab, step, out_state, out_register, done, sem):
    inner = [
        pltpu.make_async_copy(
            src.at[:, pl.ds(1, NX - 2)], dst.at[:, pl.ds(1, NX - 2)], sem.at[i, 0]
        )
        for i, (src, dst) in enumerate(((u, out_state), (k, out_register)))
    ]
    for copy in inner:
        copy.start()
    outer = []
    for side in (0, 1):
        x = 0 if side == 0 else NX - 1
        for c in range(CH):
            rows = pl.ds(ROWS * c, ROWS)
            own = [u[v, x, rows, :] for v in range(NV)]
            if c:
                far = [far_x[side, c - 1, v] for v in range(NV)]
            else:
                dt = step[:, 0:AHEAD]
                far = [
                    jnp.concatenate(
                        [far_ab[0, side, v] + dt * far_ab[1, side, v], far_rest[side, v]], axis=1
                    )
                    for v in range(NV)
                ]
            extra = x_face(side, own, far)
            for v in range(NV):
                new_k, new_u = advance(
                    1, k[v, x, rows, :], own[v], step[...], edge[side, v, rows, :] + extra[v]
                )
                done[0, side, v, rows, :] = new_u
                done[1, side, v, rows, :] = new_k
        for i, dst in enumerate((out_state, out_register)):
            copy = pltpu.make_async_copy(done.at[i, side], dst.at[:, x], sem.at[i, 1 + side])
            copy.start()
            outer.append(copy)
    for copy in inner + outer:
        copy.wait()


def shards(sizes, state, register):
    mat_z, mat_y = operators()
    nz, nxl, ny, nxh, nco = sizes
    steps_1, steps_2 = z_steps(nz)
    counts = (len(steps_1), len(steps_2) * nxh * nxl * nco - 1, ny - 1)
    block = (NV, NX, NY, NZ)
    vmem = lambda *shape: pltpu.VMEM(shape, jnp.float32)
    dma = lambda *shape: pltpu.SemaphoreType.DMA(shape)
    array = lambda *shape: jax.ShapeDtypeStruct(shape, jnp.float32)
    in_vmem = pl.BlockSpec(memory_space=pltpu.VMEM)
    in_hbm = pl.BlockSpec(memory_space=pltpu.HBM)
    parts = pl.pallas_call(
        functools.partial(kernel, sizes),
        out_shape=(
            array(*block),
            array(*block),
            array(2, NV, NY, NZ),
            array(2, CH - 1, NV, ROWS, NZ),
            array(2, NV, ROWS, NZ - AHEAD),
            array(2, 2, NV, ROWS, AHEAD),
            array(ROWS, NZ),
        ),
        in_specs=[in_hbm] * 4,
        out_specs=[in_vmem] * 7,
        scratch_shapes=[
            vmem(*block),
            vmem(*block),
            vmem(*block),
            vmem(*block),
            pltpu.VMEM((2, 2, 2 * LANES, 2 * LANES), jnp.bfloat16),
            pltpu.VMEM((2, NX * NY, NX * NY), jnp.bfloat16),
            vmem(ROWS, NZ),
            vmem(3, 1, LANES),
            vmem(counts[0], 1, LANES),
            vmem(counts[1], 1, LANES),
            vmem(counts[2], 1, LANES),
            vmem(2, 2, NV, ROWS, NZ),
            vmem(2, 2, NY, LANES),
            vmem(2, 2, NV, ROWS, NZ),
            vmem(2, 2, NY, LANES),
            vmem(2, CH, NV, ROWS, NZ),
            vmem(2, 2, NV, ROWS, AHEAD),
            vmem(2, NV, ROWS, NZ),
            vmem(2, NV, NY, LANES),
            dma(NX + 3),
            dma(2, 2, CH),
            dma(2, 2, CH),
            dma(2, 2),
            dma(2, 2),
            dma(2, 2, 2),
            dma(2, 2, 2),
            dma(sum(counts)),
            dma(sum(counts)),
        ],
        compiler_params=pltpu.CompilerParams(
            collective_id=0, has_side_effects=True, vmem_limit_bytes=32 * 2**20
        ),
        name="sections",
    )(*[pltpu.with_memory_space_constraint(x, pltpu.HBM) for x in (state, register, mat_z, mat_y)])
    return pl.pallas_call(
        finish,
        out_shape=(array(*block), array(*block)),
        in_specs=[in_vmem] * 7,
        out_specs=[in_hbm] * 2,
        scratch_shapes=[vmem(2, 2, NV, NY, NZ), dma(2, 3)],
        compiler_params=pltpu.CompilerParams(vmem_limit_bytes=16 * 2**20),
        name="finish",
    )(*parts)


def solution(mesh):
    gx, gy, gz = (mesh.shape[a] for a in ("gx", "gy", "gz"))
    sizes = (gx // 2, 2, gy, gz // 2, 2)
    torus = Mesh(mesh.devices.reshape(sizes), AXES)
    placed = P(None, ("gx_0", "gx_1"), "gy", ("gz_0", "gz_1"))
    return jax.shard_map(
        functools.partial(shards, sizes),
        mesh=torus,
        in_specs=(placed, placed),
        out_specs=(placed, placed),
        check_vma=False,
    )
```
